128 devices in a mesh: gx: 8 (over z, y_hi), gy: 8 (over x, core), lev: 2 (over y_lo).
Axes of the slice: x: 4, y: 4 (y_hi: 2, y_lo: 2; y = y_hi * 2 + y_lo), z: 4, core: 2. Of those that a mesh axis runs over, the one named last changes fastest.
Arguments:
- child_field: bfloat16 [136, 1024, 2048], P('lev', 'gx', 'gy'), may hold values from -6 to 6
- parent_old: bfloat16 [90, 1024, 2048], P('lev', 'gx', 'gy'), may hold values from -6 to 6
- level_map: int32 [136], replicated, may hold values from 0 to 89, as said below
- intersection: float32 [136], replicated, may hold values from 0.1 to 0.9
- thickness: float32 [136], replicated, may hold values from 0.5 to 5
- smooth_coef: float32 [90], P('lev'), may hold values from 0.04 to 0.24
- nest_mask: int32 [1024, 2048], P('gx', 'gy'), may hold values 0 or 1
Outputs:
- parent_new: bfloat16 [90, 1024, 2048], P('lev', 'gx', 'gy')
The draws below stay inside these ranges and needn't reach their ends.
Inputs may be any that keep to these rules, and one draw needn't show every extreme that they name: `level_map`: starts at 0, never falls, rises by at most 1 from one child level to the next, and ends at 89, so every parent level begins some child level.
All inputs are finite; a program needn't handle non-finite values. No bound on the sum of `nest_mask` on one device may be relied on, other than what follows from the above.
Results may differ from the reference program's by a relative error of at most 0.004.
Values may be sent and summed in bfloat16 or wider, within the bound.
No kernel may reach another device: no remote copies, remote signals or barrier semaphores. Data moves between devices by JAX's collectives and lax.ppermute only.
A program may use at most 128 MiB of HBM per device.

```python
import math
import jax
import jax.numpy as jnp

KC = 136
PL = 90
SMOOTH = 4
NX = 1024
NY = 2048


def draw_level_map(key, part):
    half_parent = PL // 2
    slack_steps = min(6, (KC - PL) // 2)
    early_count = half_parent - 1 + slack_steps
    late_count = PL - half_parent + slack_steps
    step_index = jnp.arange(KC - 1, dtype=jnp.int32)
    side_pick = jax.random.randint(jax.random.fold_in(key, 11), (), 0, 2).astype(jnp.int32)
    early_pick = (jax.random.permutation(jax.random.fold_in(key, 12), early_count) < half_parent - 1).astype(jnp.int32)
    late_pick = (jax.random.permutation(jax.random.fold_in(key, 13), late_count) < PL - half_parent).astype(jnp.int32)
    early_free = jnp.concatenate([early_pick, jnp.zeros((KC - 1 - early_count,), jnp.int32)])
    late_free = jnp.concatenate([jnp.zeros((KC - 1 - late_count,), jnp.int32), late_pick])
    early_fixed = (step_index < half_parent - 1).astype(jnp.int32)
    late_fixed = (step_index >= KC - 1 - (PL - half_parent)).astype(jnp.int32)
    rise_steps = jnp.where(side_pick == 0, early_fixed + late_free, early_free + late_fixed)
    levels = jnp.concatenate([jnp.zeros((1,), jnp.int32), jnp.cumsum(rise_steps).astype(jnp.int32)])
    return levels.astype(jnp.int32)


def touch_ends(drawn, key, low, high):
    longest = drawn.shape.index(max(drawn.shape))
    spots = []
    for shift in (0, 1):
        where = [jax.random.randint(jax.random.fold_in(key, axis), (), 0, length) for axis, length in enumerate(drawn.shape)]
        where[longest] = (where[longest] + shift) % drawn.shape[longest]
        spots.append(tuple(where))
    return drawn.at[spots[0]].set(low).at[spots[1]].set(high)


def shard_levels(key, extent, shards, low, top_value):
    gain = 1.0
    for dim, shards_of in shards:
        draws = jax.random.uniform(jax.random.fold_in(jax.random.fold_in(key, 6), dim), (shards_of,), jnp.float32, low / len(shards), top_value / len(shards))
        gain = gain * jnp.repeat(jnp.exp(draws), extent[dim] // shards_of).reshape((-1,) + (1,) * (len(extent) - 1 - dim))
    return gain


def noise(rng, extent, spread, most, split=(), kind=jnp.bfloat16):
    entries = jax.random.normal(rng, extent, jnp.float32) * spread
    if len(split) > 0:
        entries = shard_levels(rng, extent, split, -0.22, 0.18) * entries
    return jnp.clip(entries, min=-most, max=most).astype(kind)


def setup_inputs(seed: int = 0) -> dict:
    streams_of = jax.random.split(jax.random.key(seed), 8)
    child_field = noise(streams_of[0], (KC, NX, NY), 1.0, 6.0, ((0, 2), (1, 8), (2, 8)))
    parent_old = noise(streams_of[1], (PL, NX, NY), 1.0, 6.0, ((0, 2), (1, 8), (2, 8)))
    level_map = draw_level_map(jax.random.fold_in(streams_of[7], 71), 0)
    intersection = jnp.clip(jax.random.uniform(streams_of[3], (KC,), jnp.float32, 0.1, 0.9), 0.1, 0.9)
    thickness = jnp.clip(jnp.exp(jax.random.uniform(streams_of[4], (KC,), jnp.float32, math.log(0.5), math.log(5.0))), 0.5, 5.0)
    smooth_coef = jnp.clip(jnp.exp(math.log(0.24) - 1.7917595 * jax.random.uniform(streams_of[5], (PL,), jnp.float32) ** shard_levels(streams_of[5], (PL,), ((0, 2),), -0.2, 0.2)), 0.04, 0.24)
    nest_mask = touch_ends((jax.random.randint(streams_of[6], (NX, NY), 0, 4) < 3).astype(jnp.int32), jax.random.fold_in(streams_of[6], 1), 0, 1)
    return {"child_field": child_field, "parent_old": parent_old, "level_map": level_map, "intersection": intersection, "thickness": thickness, "smooth_coef": smooth_coef, "nest_mask": nest_mask}


def normed_weights(level_map, intersection, thickness):
    parents = jnp.arange(PL, dtype=jnp.int32)[:, None]
    upper_level = jnp.minimum(level_map + 1, PL - 1)[None, :]
    raw_weight = jnp.where(parents == level_map[None, :], intersection * thickness, 0.0)
    raw_weight = raw_weight + jnp.where(parents == upper_level, (1.0 - intersection) * thickness, 0.0)
    return (raw_weight / jnp.sum(raw_weight, axis=1, keepdims=True)).astype(jnp.bfloat16)


def reference(child_field, parent_old, level_map, intersection, thickness, smooth_coef, nest_mask):
    normed = normed_weights(level_map, intersection, thickness)
    remapped = jnp.dot(normed, child_field.reshape(KC, -1), preferred_element_type=jnp.float32)
    remapped = remapped.reshape(PL, NX, NY)
    fed_back = jnp.where(nest_mask[None] != 0, remapped, parent_old.astype(jnp.float32))
    coef = smooth_coef[:, None, None]
    for sweep in range(SMOOTH):
        padded = jnp.pad(fed_back, ((0, 0), (1, 1), (1, 1)))
        beside = padded[:, 2:, 1:-1] + padded[:, :-2, 1:-1] + padded[:, 1:-1, 2:] + padded[:, 1:-1, :-2]
        fed_back = fed_back + coef * (beside - 4.0 * fed_back)
    return fed_back.astype(jnp.bfloat16)
```

```python
import functools

import jax
import jax.numpy as jnp
from jax import lax
from jax.experimental import pallas as pl
from jax.experimental.pallas import tpu as pltpu
from jax.sharding import PartitionSpec as P

SMOOTH = 4
LANES = 128
SUB = 8
SLOT = 24
PER_TILE = 5
PER_SENT = 3
SMALL_RUNG = 1
ROW_BLOCK = 32
F32 = jnp.float32
BF16 = jnp.bfloat16
VMEM_MIB = 1 << 20


def normed_weights(level_map, intersection, thickness, parent_total):
    parents = jnp.arange(parent_total, dtype=jnp.int32)[:, None]
    upper_level = jnp.minimum(level_map + 1, parent_total - 1)[None, :]
    raw_weight = jnp.where(parents == level_map[None, :], intersection * thickness, 0.0)
    raw_weight = raw_weight + jnp.where(
        parents == upper_level, (1.0 - intersection) * thickness, 0.0
    )
    return (raw_weight / jnp.sum(raw_weight, axis=1, keepdims=True)).astype(BF16)


def pair_swap(x, axis, parity):
    route = []
    for low in range(parity, lax.axis_size(axis) - 1, 2):
        route += [(low, low + 1), (low + 1, low)]
    return lax.ppermute(x, axis, route)


def call(kernel, grid, in_specs, out_specs, out_shape, scratch=(), flops=1, limit=24):
    return pl.pallas_call(
        kernel,
        grid=grid,
        in_specs=in_specs,
        out_specs=out_specs,
        out_shape=out_shape,
        scratch_shapes=list(scratch),
        compiler_params=pltpu.CompilerParams(vmem_limit_bytes=limit * VMEM_MIB),
        cost_estimate=pl.CostEstimate(flops=flops, bytes_accessed=1 << 20, transcendentals=0),
    )


def smem():
    return pl.BlockSpec(memory_space=pltpu.SMEM)


def whole(*shape):
    return pl.BlockSpec(shape, lambda *_: (0,) * len(shape))


def partner_kernel(count, spans, weights, child, out):
    children = child.shape[0]

    def level(j, carry):
        def add(k, total):
            return total + weights[j * children + k] * child[k].astype(F32)

        zero = jnp.zeros(child.shape[1:], F32)
        out[j] = lax.fori_loop(spans[2 * j], spans[2 * j + 1], add, zero).astype(BF16)
        return carry

    lax.fori_loop(0, count, level, 0)


def scan_children(info, slots, shares, loads, stores, zero_store, parents):
    children = slots.shape[0] - 1
    zeros = [jnp.zeros_like(x) for x in loads(0)]

    def clear(p, carry):
        zero_store(p)
        return carry

    lax.fori_loop(0, info[5], clear, 0)
    lax.fori_loop(info[6], parents, clear, 0)

    def step(k, state):
        here, above = state
        rose = shares[2 * children + k]
        kept = 1.0 - rose
        low, high = shares[k], shares[children + k]
        values = loads(k)
        here = [kept * h + rose * a + low * v for h, a, v in zip(here, above, values)]
        above = [kept * a + high * v for a, v in zip(above, values)]
        stores(slots[k], here)
        return here, above

    here, above = lax.fori_loop(0, children, step, (zeros, zeros), unroll=4)
    stores(slots[children], above)


def rows_kernel(
    parents, count, info, slots, shares,
    child_t, child_b, par_t, par_b, mask_t, mask_b, part_t, part_b, even, odd, top, bot,
):
    def loads(k):
        return [child_t[k].astype(F32), child_b[k].astype(F32)]

    def stores(slot, values):
        top[slot], bot[slot] = values

    def zero_store(p):
        top[p] = jnp.zeros(top.shape[1:], F32)
        bot[p] = jnp.zeros(bot.shape[1:], F32)

    scan_children(info, slots, shares, loads, stores, zero_store, parents)

    def add_partner(j, carry):
        p = info[2] + j
        top[p] += part_t[j].astype(F32)
        bot[p] += part_b[j].astype(F32)
        return carry

    lax.fori_loop(0, count, add_partner, 0)
    row = lax.broadcasted_iota(jnp.int32, top.shape[1:], 0)
    flip = info[0] == 1
    fed_t, fed_b = mask_t[...] != 0, mask_b[...] != 0

    def pair(m, carry):
        p, q = 2 * m, jnp.minimum(2 * m + 1, parents - 1)
        tops = [jnp.where(fed_t, top[i], par_t[i].astype(F32)) for i in (p, q)]
        bots = [jnp.where(fed_b, bot[i], par_b[i].astype(F32)) for i in (p, q)]
        first = jnp.where(row < SMOOTH, tops[0], pltpu.roll(tops[1], SMOOTH, 0))
        last = jnp.where(row < SMOOTH, pltpu.roll(bots[0], SMOOTH, 0), bots[1])
        even[m] = jnp.where(flip, first, last).astype(BF16)
        odd[m] = jnp.where(flip, last, first).astype(BF16)
        return carry

    lax.fori_loop(0, even.shape[0], pair, 0, unroll=2)


def field_kernel(
    parents, count, info, slots, shares, child, par, mask, part, field, edge, sent, acc
):
    def loads(k):
        return [child[k].astype(F32)]

    def stores(slot, values):
        acc[slot] = values[0]

    def zero_store(p):
        acc[p] = jnp.zeros(acc.shape[1:], F32)

    scan_children(info, slots, shares, loads, stores, zero_store, parents)

    def add_partner(j, carry):
        acc[info[2] + j] += part[j].astype(F32)
        return carry

    lax.fori_loop(0, count, add_partner, 0)
    fed = mask[...] != 0

    def blend(p, carry):
        field[p] = jnp.where(fed, acc[p], par[p].astype(F32)).astype(BF16)
        return carry

    lax.fori_loop(0, parents, blend, 0, unroll=3)
    edges = make_edges(parents, lambda p: field[p].astype(F32))
    for t, tile in enumerate(edges):
        edge[t] = tile.astype(BF16)
    for t, tile in enumerate(make_sent(edges)):
        sent[t] = tile.astype(BF16)


def make_edges(parents, load):
    tiles = []
    for t in range(pl.cdiv(parents, PER_TILE)):
        tile = None
        for j in range(min(PER_TILE, parents - t * PER_TILE)):
            value = load(t * PER_TILE + j)
            lane = lax.broadcasted_iota(jnp.int32, (value.shape[0], LANES), 1) - SLOT * j
            last = pltpu.roll(value[:, -LANES:], (SLOT * j + 8) % LANES, 1)
            first = pltpu.roll(value[:, :LANES], (SLOT * j + 16) % LANES, 1)
            both = jnp.where(lane < 12, last, first)
            tile = both if tile is None else jnp.where(lane >= 0, both, tile)
        tiles.append(tile)
    return tiles


def make_sent(edges):
    tiles = []
    for q in range(pl.cdiv(len(edges), PER_SENT)):
        tile = None
        for u, edge in enumerate(edges[q * PER_SENT : (q + 1) * PER_SENT]):
            lane = lax.broadcasted_iota(jnp.int32, edge.shape, 1) % SLOT - 8 * u
            last = pltpu.roll(edge, (8 * u - 4) % LANES, 1)
            first = pltpu.roll(edge, (8 * u - 12) % LANES, 1)
            both = jnp.where(lane < 4, last, first)
            tile = both if tile is None else jnp.where(lane >= 0, both, tile)
        tiles.append(tile)
    return tiles


def halo_kernel(parents, info, even, odd, sent_core, halo, edge, sent):
    flip = info[0] == 1
    row = lax.broadcasted_iota(jnp.int32, halo.shape[1:], 0)

    def load(p):
        a, b = even[p // 2].astype(F32), odd[p // 2].astype(F32)
        after, before = jnp.where(flip, b, a), jnp.where(flip, a, b)
        if p % 2 == 0:
            before = pltpu.roll(before, SMOOTH, 0)
        else:
            after = pltpu.roll(after, SMOOTH, 0)
        value = jnp.where(row < SMOOTH, after, before)
        halo[p] = value.astype(BF16)
        return value

    edges = make_edges(parents, load)
    for t, tile in enumerate(edges):
        edge[t] = tile.astype(BF16)
    rows = sent_core.shape[1]
    sent[:, :rows, :] = sent_core[...]
    for t, tile in enumerate(make_sent(edges)):
        sent[t, rows:, :] = tile.astype(BF16)


def row_sweep(values, side_sum, scales, keeps):
    count = len(values)
    before = pltpu.roll(values[-1], 1, 0)
    after = pltpu.roll(values[0], SUB - 1, 0)
    out = []
    for i, value in enumerate(values):
        up = values[i - 1] if i > 0 else before
        down = values[i + 1] if i < count - 1 else after
        out.append(keeps[i] * value + scales[i] * ((up + down) + side_sum(i, value)))
    return out


def row_flags(info, count, rows):
    sub = lax.broadcasted_iota(jnp.int32, (SUB, LANES), 0)
    flags = []
    for i in range(count):
        r = (SUB - 1) * count + i - rows
        if r < 0:
            flags.append(None)
            continue
        inside = info[4] if r < SMOOTH else info[3]
        flags.append(jnp.where(sub == SUB - 1, inside.astype(F32), 1.0))
    return flags


def smooth_kernel(info, coefs, field, halo, out, left, right):
    levels, rows = field.shape[:2]
    count = left.shape[0] // SUB
    lane = lax.broadcasted_iota(jnp.int32, (SUB, LANES), 1)
    flags = row_flags(info, count, rows)
    base = pl.program_id(0) * levels

    def level(p, carry):
        scale = coefs[base + p]
        keep = 1.0 - 4.0 * scale
        scales = [scale if f is None else scale * f for f in flags]
        keeps = [keep if f is None else keep * f for f in flags]
        for ref, cut in ((left, slice(0, LANES)), (right, slice(LANES, 2 * LANES))):
            ref[:rows, :] = field[p, :, cut].astype(F32)
            ref[rows:, :] = halo[p, :, cut].astype(F32)
        a = [left[pl.ds(i, SUB, stride=count), :] for i in range(count)]
        b = [right[pl.ds(i, SUB, stride=count), :] for i in range(count)]
        for _ in range(SMOOTH):
            ups = [(pltpu.roll(x, 1, 1), pltpu.roll(y, 1, 1)) for x, y in zip(a, b)]
            dns = [
                (pltpu.roll(x, LANES - 1, 1), pltpu.roll(y, LANES - 1, 1)) for x, y in zip(a, b)
            ]
            sides = [
                (ua + jnp.where(lane == LANES - 1, db, da), jnp.where(lane == 0, ua, ub) + db)
                for (ua, ub), (da, db) in zip(ups, dns)
            ]
            a = row_sweep(a, lambda i, _: sides[i][0], scales, keeps)
            b = row_sweep(b, lambda i, _: sides[i][1], scales, keeps)
        for i in range(count):
            left[pl.ds(i, SUB, stride=count), :] = a[i]
            right[pl.ds(i, SUB, stride=count), :] = b[i]
        out[p, :, :LANES] = left[:rows, :].astype(BF16)
        out[p, :, LANES:] = right[:rows, :].astype(BF16)
        return carry

    lax.fori_loop(0, levels, level, 0)


def seam_kernel(info, coefs, even, odd, core, edge, main, out, tiles, work):
    total = tiles.shape[0]
    rows = core.shape[1]
    count = tiles.shape[1] // SUB
    step = pl.program_id(0)

    @pl.when(step == 0)
    def _():
        flip = info[1] == 1
        flags = row_flags(info, count, rows)
        slot = lax.broadcasted_iota(jnp.int32, tiles.shape[1:], 1) % SLOT
        for q in range(even.shape[0]):
            a, b = even[q].astype(F32), odd[q].astype(F32)
            after, before = jnp.where(flip, b, a), jnp.where(flip, a, b)
            for u in range(min(PER_SENT, total - q * PER_SENT)):
                t = q * PER_SENT + u
                own = jnp.concatenate([core[t].astype(F32), edge[t].astype(F32)], axis=0)
                right = pltpu.roll(after, (4 - 8 * u) % LANES, 1)
                left = pltpu.roll(before, (12 - 8 * u) % LANES, 1)
                tile = jnp.where(slot < 12, right, left)
                tiles[t] = jnp.where((slot >= 8) & (slot < 16), tile, own)
        for t in range(total):
            for i in range(count):
                work[0, t, i] = tiles[t, pl.ds(i, SUB, stride=count), :]
        for s in range(SMOOTH):
            for t in range(total):
                scale = coefs[0, t]
                keep = coefs[1, t]
                scales = [scale if f is None else scale * f for f in flags]
                keeps = [keep if f is None else keep * f for f in flags]
                values = [work[s % 2, t, i] for i in range(count)]
                new = row_sweep(
                    values,
                    lambda _, x: pltpu.roll(x, 1, 1) + pltpu.roll(x, LANES - 1, 1),
                    scales,
                    keeps,
                )
                for i in range(count):
                    if s < SMOOTH - 1:
                        work[(s + 1) % 2, t, i] = new[i]
                    else:
                        tiles[t, pl.ds(i, SUB, stride=count), :] = new[i]

    seam = tiles[step, :rows, :]
    lane = lax.broadcasted_iota(jnp.int32, seam.shape, 1)
    for j in range(main.shape[0]):
        first = pltpu.roll(seam, (-SLOT * j - 16) % LANES, 1)
        last = pltpu.roll(seam, (120 - SLOT * j) % LANES, 1)
        a, b = main[j, :, :LANES].astype(F32), main[j, :, LANES:].astype(F32)
        out[j, :, :LANES] = jnp.where(lane < SMOOTH, first, a).astype(BF16)
        out[j, :, LANES:] = jnp.where(lane >= LANES - SMOOTH, last, b).astype(BF16)


def feed_back(count, child, parent, normed, level_map, smooth_coef, mask):
    children, rows, columns = child.shape
    parents = parent.shape[0]
    total = normed.shape[0]
    slab = lax.axis_index("lev")
    gx, gy = lax.axis_index("gx"), lax.axis_index("gy")
    own_map = lax.dynamic_slice_in_dim(level_map, slab * children, children)
    own = lax.dynamic_slice_in_dim(normed, slab * children, children, 1).astype(F32)
    levels = jnp.arange(total, dtype=jnp.int32)[:, None]
    low = jnp.sum(jnp.where(levels == own_map, own, 0.0), axis=0)
    high = jnp.sum(jnp.where(levels == own_map + 1, own, 0.0), axis=0)
    rose = jnp.concatenate([jnp.zeros((1,), F32), (own_map[1:] != own_map[:-1]).astype(F32)])
    shares = jnp.concatenate([low, high, rose])
    place = jnp.concatenate([own_map, own_map[-1:] + 1]) - slab * parents
    slots = jnp.where((place >= 0) & (place < parents), place, parents)
    start = jnp.where(slab == 0, parents, parents - count)
    window = start + jnp.arange(count, dtype=jnp.int32)[:, None]
    spans = jnp.concatenate(
        [
            jnp.sum((own_map < window - 1).astype(jnp.int32), axis=1, keepdims=True),
            jnp.sum((own_map <= window).astype(jnp.int32), axis=1, keepdims=True),
        ],
        axis=1,
    ).reshape(-1)
    weights = lax.dynamic_slice_in_dim(own, start, count, 0).reshape(-1)
    info = jnp.stack(
        [
            gx % 2,
            gy % 2,
            jnp.where(slab == 0, parents - count, 0),
            (gx > 0).astype(jnp.int32),
            (gx < lax.axis_size("gx") - 1).astype(jnp.int32),
            jnp.clip(place[0], 0, parents),
            jnp.clip(place[-1] + 1, 0, parents),
        ]
    ).astype(jnp.int32)

    block = ROW_BLOCK
    part = call(
        functools.partial(partner_kernel, count),
        (rows // block,),
        [smem(), smem(), pl.BlockSpec((children, block, columns), lambda i: (0, i, 0))],
        pl.BlockSpec((count, block, columns), lambda i: (0, i, 0)),
        jax.ShapeDtypeStruct((count, rows, columns), BF16),
    )(spans, weights, child)
    part = pair_swap(part, "lev", 0)

    ends = rows // SUB - 1

    def two(lead):
        return [
            pl.BlockSpec((lead, SUB, columns), lambda i: (0, 0, 0)),
            pl.BlockSpec((lead, SUB, columns), lambda i: (0, ends, 0)),
        ]

    packed = pl.cdiv(parents, 2)
    strip = jax.ShapeDtypeStruct((packed, SUB, columns), BF16)
    row_even, row_odd = call(
        functools.partial(rows_kernel, parents, count),
        (1,),
        [
            smem(), smem(), smem(),
            *two(children),
            *two(parents),
            pl.BlockSpec((SUB, columns), lambda i: (0, 0)),
            pl.BlockSpec((SUB, columns), lambda i: (ends, 0)),
            *two(count),
        ],
        [whole(packed, SUB, columns)] * 2,
        [strip, strip],
        [pltpu.VMEM((parents + 1, SUB, columns), F32)] * 2,
    )(info, slots, shares, child, child, parent, parent, mask, mask, part, part)
    row_even = pair_swap(row_even, "gx", 0)
    row_odd = pair_swap(row_odd, "gx", 1)

    seams = pl.cdiv(parents, PER_TILE)
    sents = pl.cdiv(seams, PER_SENT)
    field, edge_core, sent_core = call(
        functools.partial(field_kernel, parents, count),
        (rows // block,),
        [
            smem(), smem(), smem(),
            pl.BlockSpec((children, block, columns), lambda i: (0, i, 0)),
            pl.BlockSpec((parents, block, columns), lambda i: (0, i, 0)),
            pl.BlockSpec((block, columns), lambda i: (i, 0)),
            pl.BlockSpec((count, block, columns), lambda i: (0, i, 0)),
        ],
        [
            pl.BlockSpec((parents, block, columns), lambda i: (0, i, 0)),
            pl.BlockSpec((seams, block, LANES), lambda i: (0, i, 0)),
            pl.BlockSpec((sents, block, LANES), lambda i: (0, i, 0)),
        ],
        [
            jax.ShapeDtypeStruct((parents, rows, columns), BF16),
            jax.ShapeDtypeStruct((seams, rows, LANES), BF16),
            jax.ShapeDtypeStruct((sents, rows, LANES), BF16),
        ],
        [pltpu.VMEM((parents + 1, block, columns), F32)],
        flops=1 << 34,
    )(info, slots, shares, child, parent, mask, part)

    extended = rows + SUB
    halo, edge_halo, sent = call(
        functools.partial(halo_kernel, parents),
        (1,),
        [smem(), whole(packed, SUB, columns), whole(packed, SUB, columns), whole(sents, rows, LANES)],
        [whole(parents, SUB, columns), whole(seams, SUB, LANES), whole(sents, extended, LANES)],
        [
            jax.ShapeDtypeStruct((parents, SUB, columns), BF16),
            jax.ShapeDtypeStruct((seams, SUB, LANES), BF16),
            jax.ShapeDtypeStruct((sents, extended, LANES), BF16),
        ],
    )(info, row_even, row_odd, sent_core)
    column_even = pair_swap(sent, "gy", 0)
    column_odd = pair_swap(sent, "gy", 1)

    group = PER_TILE
    main = call(
        smooth_kernel,
        (parents // group,),
        [
            smem(), smem(),
            pl.BlockSpec((group, rows, columns), lambda i: (i, 0, 0)),
            pl.BlockSpec((group, SUB, columns), lambda i: (i, 0, 0)),
        ],
        pl.BlockSpec((group, rows, columns), lambda i: (i, 0, 0)),
        jax.ShapeDtypeStruct((parents, rows, columns), BF16),
        [pltpu.VMEM((extended, LANES), F32)] * 2,
        flops=1 << 34,
    )(info, smooth_coef, field, halo)

    lane = jnp.arange(LANES, dtype=jnp.int32)
    place_in_slot = lane % SLOT
    inside = lane < SLOT * PER_TILE
    after = (place_in_slot >= 8) & (place_in_slot < 12)
    before = (place_in_slot >= 12) & (place_in_slot < 16)
    inside &= ~after | (gy < lax.axis_size("gy") - 1)
    inside &= ~before | (gy > 0)
    by_tile = jnp.repeat(smooth_coef.reshape(seams, PER_TILE), SLOT, axis=1)
    by_tile = jnp.pad(by_tile, ((0, 0), (0, LANES - SLOT * PER_TILE)))
    lane_coefs = jnp.where(inside, jnp.stack([by_tile, 1.0 - 4.0 * by_tile]), 0.0)
    lane_coefs = jnp.broadcast_to(lane_coefs[:, :, None, :], (2, seams, SUB, LANES))
    return call(
        seam_kernel,
        (seams,),
        [
            smem(),
            whole(2, seams, SUB, LANES),
            whole(sents, extended, LANES),
            whole(sents, extended, LANES),
            whole(seams, rows, LANES),
            whole(seams, SUB, LANES),
            pl.BlockSpec((group, rows, columns), lambda i: (i, 0, 0)),
        ],
        pl.BlockSpec((group, rows, columns), lambda i: (i, 0, 0)),
        jax.ShapeDtypeStruct((parents, rows, columns), BF16),
        [
            pltpu.VMEM((seams, extended, LANES), F32),
            pltpu.VMEM((2, seams, extended // SUB, SUB, LANES), F32),
        ],
    )(info, lane_coefs, column_even, column_odd, edge_core, edge_halo, main)


def shards(child_field, parent_old, level_map, intersection, thickness, smooth_coef, nest_mask):
    children, parents = child_field.shape[0], parent_old.shape[0]
    total = parents * lax.axis_size("lev")
    normed = normed_weights(level_map, intersection, thickness, total)
    most = children - parents + 1
    crossing = jnp.maximum(level_map[children - 1] + 2 - parents, parents - level_map[children])

    def run(count):
        return lambda: feed_back(
            count, child_field, parent_old, normed, level_map, smooth_coef, nest_mask
        )

    return lax.cond(crossing <= SMALL_RUNG, run(SMALL_RUNG), run(most))


def solution(mesh):
    in_specs = (P("lev", "gx", "gy"), P("lev", "gx", "gy"), P(), P(), P(), P("lev"), P("gx", "gy"))
    out_specs = P("lev", "gx", "gy")
    return jax.shard_map(shards, mesh=mesh, in_specs=in_specs, out_specs=out_specs, check_vma=False)
```

```python
import functools

import jax
import jax.numpy as jnp
from jax import lax
from jax.experimental import pallas as pl
from jax.experimental.pallas import tpu as pltpu
from jax.sharding import PartitionSpec as P

SMOOTH = 4
LANES = 128
SUB = 8
SLOT = 24
PER_TILE = 5
PER_SENT = 3
SMALL_RUNG = 1
ROW_BLOCK = 32
F32 = jnp.float32
BF16 = jnp.bfloat16
VMEM_MIB = 1 << 20


def pair_swap(x, axis, parity):
    route = []
    for low in range(parity, lax.axis_size(axis) - 1, 2):
        route += [(low, low + 1), (low + 1, low)]
    return lax.ppermute(x, axis, route)


def call(kernel, grid, in_specs, out_specs, out_shape, scratch=(), flops=1, limit=24):
    return pl.pallas_call(
        kernel,
        grid=grid,
        in_specs=in_specs,
        out_specs=out_specs,
        out_shape=out_shape,
        scratch_shapes=list(scratch),
        compiler_params=pltpu.CompilerParams(vmem_limit_bytes=limit * VMEM_MIB),
        cost_estimate=pl.CostEstimate(flops=flops, bytes_accessed=1 << 20, transcendentals=0),
    )


def smem():
    return pl.BlockSpec(memory_space=pltpu.SMEM)


def whole(*shape):
    return pl.BlockSpec(shape, lambda *_: (0,) * len(shape))


def deal_column(row, size):
    r = lax.broadcasted_iota(jnp.int32, (size, size), 0)
    c = lax.broadcasted_iota(jnp.int32, (size, size), 1)
    return jnp.sum(jnp.where(r == c, row, 0.0), axis=1, keepdims=True)


def share_columns(table, size, total):
    begins, inside, thick = (deal_column(table[i : i + 1, :size], size) for i in range(3))
    parent = lax.broadcasted_iota(jnp.int32, (size, LANES), 1).astype(F32)
    raw = jnp.where(parent == begins, inside * thick, 0.0)
    upper = jnp.minimum(begins + 1.0, total - 1.0)
    raw = raw + jnp.where(parent == upper, (1.0 - inside) * thick, 0.0)
    sums = jnp.where(parent < total, jnp.sum(raw, axis=0, keepdims=True), 1.0)
    normed = (raw / sums).astype(BF16).astype(F32)
    low = jnp.sum(jnp.where(parent == begins, normed, 0.0), axis=1, keepdims=True)
    high = jnp.sum(jnp.where(parent == begins + 1.0, normed, 0.0), axis=1, keepdims=True)
    return low, high


def remap_kernel(count, total, info, begins, table, child, par, mask, field, part, acc, low, high):
    children, parents = child.shape[0], field.shape[0]
    size, width = low.shape

    @pl.when(pl.program_id(0) == 0)
    def _():
        below, above = share_columns(table, size, total)
        low[...] = jnp.broadcast_to(below, low.shape)
        high[...] = jnp.broadcast_to(above, high.shape)

    slab = info[7]
    origin = slab * children
    trash = parents + count
    first = begins[origin] - slab * parents
    last = begins[origin + children - 1] - slab * parents

    def clear(p, carry):
        acc[p] = jnp.zeros(acc.shape[1:], F32)
        return carry

    lax.fori_loop(0, jnp.maximum(first, 0), clear, 0)
    untouched = jnp.where(slab == 0, last + 2, parents)
    end = parents + jnp.where(slab == 0, count, jnp.clip(first + count, 0, count))
    lax.fori_loop(untouched, end, clear, 0)

    def step(k, state):
        here, above = state
        level = begins[origin + k]
        rose = level != begins[jnp.maximum(origin + k - 1, 0)]
        value = child[k].astype(F32)
        here = jnp.where(rose, above, here) + low[pl.ds(origin + k, 1), :] * value
        above = jnp.where(rose, 0.0, above) + high[pl.ds(origin + k, 1), :] * value
        place = level - slab * parents
        place = jnp.where(place >= 0, place, parents + count + place)
        acc[jnp.clip(place, 0, trash)] = here
        return here, above

    zero = jnp.zeros(acc.shape[1:], F32)
    here, above = lax.fori_loop(0, children, step, (zero, zero), unroll=4)
    acc[jnp.where(slab == 0, jnp.clip(last + 1, 0, trash), trash)] = above
    fed = mask[...] != 0

    def blend(p, carry):
        field[p] = jnp.where(fed, acc[p], par[p].astype(F32)).astype(BF16)
        return carry

    lax.fori_loop(0, parents, blend, 0, unroll=5)

    def pass_on(j, carry):
        part[j] = acc[parents + j].astype(BF16)
        return carry

    lax.fori_loop(0, count, pass_on, 0)


def rows_kernel(count, info, field_t, field_b, mask_t, mask_b, part_t, part_b, even, odd, top, bot):
    parents = field_t.shape[0]
    row = lax.broadcasted_iota(jnp.int32, field_t.shape[1:], 0)
    flip = info[0] == 1
    fed_t, fed_b = mask_t[...] != 0, mask_b[...] != 0

    def copy(p, carry):
        top[p] = field_t[p].astype(F32)
        bot[p] = field_b[p].astype(F32)
        return carry

    lax.fori_loop(0, parents, copy, 0, unroll=9)

    def add_partner(j, carry):
        p = info[2] + j
        top[p] += jnp.where(fed_t, part_t[j].astype(F32), 0.0)
        bot[p] += jnp.where(fed_b, part_b[j].astype(F32), 0.0)
        return carry

    lax.fori_loop(0, count, add_partner, 0)
    for m in range(even.shape[0]):
        p, q = 2 * m, min(2 * m + 1, parents - 1)
        first = jnp.where(row < SMOOTH, top[p], pltpu.roll(top[q], SMOOTH, 0))
        last = jnp.where(row < SMOOTH, pltpu.roll(bot[p], SMOOTH, 0), bot[q])
        even[m] = jnp.where(flip, first, last).astype(BF16)
        odd[m] = jnp.where(flip, last, first).astype(BF16)


def edge_kernel(count, info, field, mask, part, fixed, edge, sent):
    parents = field.shape[0]
    fed = mask[...] != 0

    def fix(j, carry):
        value = field[info[2] + j].astype(F32) + jnp.where(fed, part[j].astype(F32), 0.0)
        fixed[j] = value.astype(BF16)
        return carry

    lax.fori_loop(0, count, fix, 0)

    def load(p):
        value = field[p].astype(F32)
        for start, near in ((0, p < count), (parents - count, p >= parents - count)):
            if near:
                mine = info[2] == start
                value = jnp.where(mine, fixed[p - start].astype(F32), value)
        return value

    edges = make_edges(parents, load)
    for t, tile in enumerate(edges):
        edge[t] = tile.astype(BF16)
    for t, tile in enumerate(make_sent(edges)):
        sent[t] = tile.astype(BF16)


def make_edges(parents, load):
    tiles = []
    for t in range(pl.cdiv(parents, PER_TILE)):
        tile = None
        for j in range(min(PER_TILE, parents - t * PER_TILE)):
            value = load(t * PER_TILE + j)
            lane = lax.broadcasted_iota(jnp.int32, (value.shape[0], LANES), 1)
            both = jnp.where(lane < LANES // 2, value[:, :LANES], value[:, -LANES:])
            both = pltpu.roll(both, (SLOT * j + 8) % LANES, 1)
            tile = both if tile is None else jnp.where(lane >= SLOT * j, both, tile)
        tiles.append(jnp.where(lane % SLOT < 8, tile, pltpu.roll(tile, 8, 1)))
    return tiles


def make_sent(edges):
    tiles = []
    for q in range(pl.cdiv(len(edges), PER_SENT)):
        tile = None
        for u, edge in enumerate(edges[q * PER_SENT : (q + 1) * PER_SENT]):
            lane = lax.broadcasted_iota(jnp.int32, edge.shape, 1) % SLOT - 8 * u
            last = pltpu.roll(edge, (8 * u - 4) % LANES, 1)
            first = pltpu.roll(edge, (8 * u - 12) % LANES, 1)
            both = jnp.where(lane < 4, last, first)
            tile = both if tile is None else jnp.where(lane >= 0, both, tile)
        tiles.append(tile)
    return tiles


def halo_kernel(parents, info, even, odd, sent_core, halo, edge, sent):
    flip = info[0] == 1
    row = lax.broadcasted_iota(jnp.int32, halo.shape[1:], 0)

    def load(p):
        a, b = even[p // 2].astype(F32), odd[p // 2].astype(F32)
        after, before = jnp.where(flip, b, a), jnp.where(flip, a, b)
        if p % 2 == 0:
            before = pltpu.roll(before, SMOOTH, 0)
        else:
            after = pltpu.roll(after, SMOOTH, 0)
        value = jnp.where(row < SMOOTH, after, before)
        halo[p] = value.astype(BF16)
        return value

    edges = make_edges(parents, load)
    for t, tile in enumerate(edges):
        edge[t] = tile.astype(BF16)
    rows = sent_core.shape[1]
    sent[:, :rows, :] = sent_core[...]
    for t, tile in enumerate(make_sent(edges)):
        sent[t, rows:, :] = tile.astype(BF16)


def row_sweep(values, side_sum, scales, keeps):
    count = len(values)
    before = pltpu.roll(values[-1], 1, 0)
    after = pltpu.roll(values[0], SUB - 1, 0)
    out = []
    for i, value in enumerate(values):
        up = values[i - 1] if i > 0 else before
        down = values[i + 1] if i < count - 1 else after
        out.append(keeps[i] * value + scales[i] * ((up + down) + side_sum(i, value)))
    return out


def row_flags(info, count, rows):
    sub = lax.broadcasted_iota(jnp.int32, (SUB, LANES), 0)
    flags = []
    for i in range(count):
        r = (SUB - 1) * count + i - rows
        if r < 0:
            flags.append(None)
            continue
        inside = info[4] if r < SMOOTH else info[3]
        flags.append(jnp.where(sub == SUB - 1, inside.astype(F32), 1.0))
    return flags


def smooth_kernel(count, info, coefs, field, fixed, halo, out, left, right, work, sides, near):
    levels, rows = field.shape[:2]
    deals = left.shape[1] // SUB
    flags = row_flags(info, deals, rows)
    flags = [None if f is None else jnp.concatenate([f, f], axis=1) for f in flags]
    base = pl.program_id(0) * levels

    @pl.when(pl.program_id(0) == 0)
    def _():
        r = lax.broadcasted_iota(jnp.int32, near.shape, 0)
        c = lax.broadcasted_iota(jnp.int32, near.shape, 1)
        near[...] = jnp.where(jnp.abs(r - c) == 1, 1.0, 0.0).astype(BF16)

    weights = []
    for p in range(levels):
        scale = coefs[base + p]
        keep = 1.0 - 4.0 * scale
        weights.append(
            (
                [scale if f is None else scale * f for f in flags],
                [keep if f is None else keep * f for f in flags],
            )
        )
        j = base + p - info[2]
        use_fixed = (j >= 0) & (j < count)
        j = jnp.clip(j, 0, count - 1)
        for ref, cut in ((left, slice(0, LANES)), (right, slice(LANES, 2 * LANES))):
            ref[p, :rows, :] = field[p, :, cut].astype(F32)

            @pl.when(use_fixed)
            def _():
                ref[p, :rows, :] = fixed[j, :, cut].astype(F32)

            ref[p, rows:, :] = halo[p, :, cut].astype(F32)
        for i in range(deals):
            part = slice(SUB * i, SUB * i + SUB)
            work[0, p, part, :LANES] = left[p, pl.ds(i, SUB, stride=deals), :]
            work[0, p, part, LANES:] = right[p, pl.ds(i, SUB, stride=deals), :]
    for s in range(SMOOTH):
        flat = work[s % 2].reshape(levels * deals * SUB, 2 * LANES).astype(BF16)
        side = jnp.dot(flat, near[...], preferred_element_type=F32)
        sides[...] = side.reshape(sides.shape)
        for p in range(levels):
            values = [work[s % 2, p, SUB * i : SUB * i + SUB, :] for i in range(deals)]
            values = row_sweep(
                values, lambda i, _: sides[p, SUB * i : SUB * i + SUB, :], *weights[p]
            )
            for i, value in enumerate(values):
                if s == SMOOTH - 1:
                    left[p, pl.ds(i, SUB, stride=deals), :] = value[:, :LANES]
                    right[p, pl.ds(i, SUB, stride=deals), :] = value[:, LANES:]
                else:
                    work[(s + 1) % 2, p, SUB * i : SUB * i + SUB, :] = value
    for p in range(levels):
        out[p, :, :LANES] = left[p, :rows, :].astype(BF16)
        out[p, :, LANES:] = right[p, :rows, :].astype(BF16)


def seam_kernel(info, coefs, even, odd, core, edge, main, out, tiles, work):
    total = tiles.shape[0]
    rows = core.shape[1]
    count = tiles.shape[1] // SUB
    step = pl.program_id(0)

    @pl.when(step == 0)
    def _():
        flip = info[1] == 1
        flags = row_flags(info, count, rows)
        slot = lax.broadcasted_iota(jnp.int32, tiles.shape[1:], 1) % SLOT
        for q in range(even.shape[0]):
            a, b = even[q].astype(F32), odd[q].astype(F32)
            after, before = jnp.where(flip, b, a), jnp.where(flip, a, b)
            for u in range(min(PER_SENT, total - q * PER_SENT)):
                t = q * PER_SENT + u
                own = jnp.concatenate([core[t].astype(F32), edge[t].astype(F32)], axis=0)
                right = pltpu.roll(after, (4 - 8 * u) % LANES, 1)
                left = pltpu.roll(before, (12 - 8 * u) % LANES, 1)
                tile = jnp.where(slot < 12, right, left)
                tiles[t] = jnp.where((slot >= 8) & (slot < 16), tile, own)
        for t in range(total):
            for i in range(count):
                work[0, t, i] = tiles[t, pl.ds(i, SUB, stride=count), :]
        for s in range(SMOOTH):
            for t in range(total):
                scale = coefs[0, t]
                keep = coefs[1, t]
                scales = [scale if f is None else scale * f for f in flags]
                keeps = [keep if f is None else keep * f for f in flags]
                values = [work[s % 2, t, i] for i in range(count)]
                new = row_sweep(
                    values,
                    lambda _, x: pltpu.roll(x, 1, 1) + pltpu.roll(x, LANES - 1, 1),
                    scales,
                    keeps,
                )
                for i in range(count):
                    if s < SMOOTH - 1:
                        work[(s + 1) % 2, t, i] = new[i]
                    else:
                        tiles[t, pl.ds(i, SUB, stride=count), :] = new[i]

    seam = tiles[step, :rows, :]
    lane = lax.broadcasted_iota(jnp.int32, seam.shape, 1)
    seam = jnp.where(lane % SLOT < 8, seam, pltpu.roll(seam, LANES - 8, 1))
    for j in range(main.shape[0]):
        first = last = pltpu.roll(seam, (120 - SLOT * j) % LANES, 1)
        a, b = main[j, :, :LANES].astype(F32), main[j, :, LANES:].astype(F32)
        out[j, :, :LANES] = jnp.where(lane < SMOOTH, first, a).astype(BF16)
        out[j, :, LANES:] = jnp.where(lane >= LANES - SMOOTH, last, b).astype(BF16)


def feed_back(count, child, parent, table, level_map, smooth_coef, mask):
    children, rows, columns = child.shape
    parents = parent.shape[0]
    total = parents * lax.axis_size("lev")
    size = level_map.shape[0]
    slab = lax.axis_index("lev")
    gx, gy = lax.axis_index("gx"), lax.axis_index("gy")
    info = jnp.stack(
        [
            gx % 2,
            gy % 2,
            jnp.where(slab == 0, parents - count, 0),
            (gx > 0).astype(jnp.int32),
            (gx < lax.axis_size("gx") - 1).astype(jnp.int32),
            (gy > 0).astype(jnp.int32),
            (gy < lax.axis_size("gy") - 1).astype(jnp.int32),
            slab,
        ]
    ).astype(jnp.int32)

    block = ROW_BLOCK
    field, part = call(
        functools.partial(remap_kernel, count, total),
        (rows // block,),
        [
            smem(), smem(), whole(*table.shape),
            pl.BlockSpec((children, block, columns), lambda i: (0, i, 0)),
            pl.BlockSpec((parents, block, columns), lambda i: (0, i, 0)),
            pl.BlockSpec((block, columns), lambda i: (i, 0)),
        ],
        [
            pl.BlockSpec((parents, block, columns), lambda i: (0, i, 0)),
            pl.BlockSpec((count, block, columns), lambda i: (0, i, 0)),
        ],
        [
            jax.ShapeDtypeStruct((parents, rows, columns), BF16),
            jax.ShapeDtypeStruct((count, rows, columns), BF16),
        ],
        [pltpu.VMEM((parents + count + 1, block, columns), F32)]
        + [pltpu.VMEM((size, columns), F32)] * 2,
    )(info, level_map, table, child, parent, mask)
    part = pair_swap(part, "lev", 0)

    ends = rows // SUB - 1

    def two(lead):
        return [
            pl.BlockSpec((lead, SUB, columns), lambda i: (0, 0, 0)),
            pl.BlockSpec((lead, SUB, columns), lambda i: (0, ends, 0)),
        ]

    packed = pl.cdiv(parents, 2)
    strip = jax.ShapeDtypeStruct((packed, SUB, columns), BF16)
    row_even, row_odd = call(
        functools.partial(rows_kernel, count),
        (1,),
        [
            smem(),
            *two(parents),
            pl.BlockSpec((SUB, columns), lambda i: (0, 0)),
            pl.BlockSpec((SUB, columns), lambda i: (ends, 0)),
            *two(count),
        ],
        [whole(packed, SUB, columns)] * 2,
        [strip, strip],
        [pltpu.VMEM((parents, SUB, columns), F32)] * 2,
    )(info, field, field, mask, mask, part, part)
    row_even = pair_swap(row_even, "gx", 0)
    row_odd = pair_swap(row_odd, "gx", 1)

    seams = pl.cdiv(parents, PER_TILE)
    sents = pl.cdiv(seams, PER_SENT)
    fixed, edge_core, sent_core = call(
        functools.partial(edge_kernel, count),
        (rows // block,),
        [
            smem(),
            pl.BlockSpec((parents, block, columns), lambda i: (0, i, 0)),
            pl.BlockSpec((block, columns), lambda i: (i, 0)),
            pl.BlockSpec((count, block, columns), lambda i: (0, i, 0)),
        ],
        [
            pl.BlockSpec((count, block, columns), lambda i: (0, i, 0)),
            pl.BlockSpec((seams, block, LANES), lambda i: (0, i, 0)),
            pl.BlockSpec((sents, block, LANES), lambda i: (0, i, 0)),
        ],
        [
            jax.ShapeDtypeStruct((count, rows, columns), BF16),
            jax.ShapeDtypeStruct((seams, rows, LANES), BF16),
            jax.ShapeDtypeStruct((sents, rows, LANES), BF16),
        ],
        flops=1 << 34,
    )(info, field, mask, part)

    extended = rows + SUB
    halo, edge_halo, sent = call(
        functools.partial(halo_kernel, parents),
        (1,),
        [smem(), whole(packed, SUB, columns), whole(packed, SUB, columns), whole(sents, rows, LANES)],
        [whole(parents, SUB, columns), whole(seams, SUB, LANES), whole(sents, extended, LANES)],
        [
            jax.ShapeDtypeStruct((parents, SUB, columns), BF16),
            jax.ShapeDtypeStruct((seams, SUB, LANES), BF16),
            jax.ShapeDtypeStruct((sents, extended, LANES), BF16),
        ],
    )(info, row_even, row_odd, sent_core)
    column_even = pair_swap(sent, "gy", 0)
    column_odd = pair_swap(sent, "gy", 1)

    group = PER_TILE
    main = call(
        functools.partial(smooth_kernel, count),
        (parents // group,),
        [
            smem(), smem(),
            pl.BlockSpec((group, rows, columns), lambda i: (i, 0, 0)),
            whole(count, rows, columns),
            pl.BlockSpec((group, SUB, columns), lambda i: (i, 0, 0)),
        ],
        pl.BlockSpec((group, rows, columns), lambda i: (i, 0, 0)),
        jax.ShapeDtypeStruct((parents, rows, columns), BF16),
        [pltpu.VMEM((group, extended, LANES), F32)] * 2
        + [
            pltpu.VMEM((2, group, extended, columns), F32),
            pltpu.VMEM((group, extended, columns), F32),
            pltpu.VMEM((columns, columns), BF16),
        ],
        flops=1 << 34,
    )(info, smooth_coef, field, fixed, halo)

    lane = jnp.arange(LANES, dtype=jnp.int32)
    place_in_slot = lane % SLOT
    inside = lane < SLOT * PER_TILE
    after = (place_in_slot >= 8) & (place_in_slot < 12)
    before = (place_in_slot >= 12) & (place_in_slot < 16)
    inside &= ~after | (gy < lax.axis_size("gy") - 1)
    inside &= ~before | (gy > 0)
    by_tile = jnp.repeat(smooth_coef.reshape(seams, PER_TILE), SLOT, axis=1)
    by_tile = jnp.pad(by_tile, ((0, 0), (0, LANES - SLOT * PER_TILE)))
    lane_coefs = jnp.where(inside, jnp.stack([by_tile, 1.0 - 4.0 * by_tile]), 0.0)
    lane_coefs = jnp.broadcast_to(lane_coefs[:, :, None, :], (2, seams, SUB, LANES))
    return call(
        seam_kernel,
        (seams,),
        [
            smem(),
            whole(2, seams, SUB, LANES),
            whole(sents, extended, LANES),
            whole(sents, extended, LANES),
            whole(seams, rows, LANES),
            whole(seams, SUB, LANES),
            pl.BlockSpec((group, rows, columns), lambda i: (i, 0, 0)),
        ],
        pl.BlockSpec((group, rows, columns), lambda i: (i, 0, 0)),
        jax.ShapeDtypeStruct((parents, rows, columns), BF16),
        [
            pltpu.VMEM((seams, extended, LANES), F32),
            pltpu.VMEM((2, seams, extended // SUB, SUB, LANES), F32),
        ],
    )(info, lane_coefs, column_even, column_odd, edge_core, edge_halo, main)


def shards(child_field, parent_old, level_map, intersection, thickness, smooth_coef, nest_mask):
    children, parents = child_field.shape[0], parent_old.shape[0]
    most = children - parents + 1
    crossing = jnp.maximum(level_map[children - 1] + 2 - parents, parents - level_map[children])
    table = jnp.stack([level_map.astype(F32), intersection, thickness])
    table = jnp.pad(table, ((0, SUB - 3), (0, -level_map.shape[0] % LANES)))

    def run(count):
        return lambda: feed_back(
            count, child_field, parent_old, table, level_map, smooth_coef, nest_mask
        )

    return lax.cond(crossing <= SMALL_RUNG, run(SMALL_RUNG), run(most))


def solution(mesh):
    in_specs = (P("lev", "gx", "gy"), P("lev", "gx", "gy"), P(), P(), P(), P("lev"), P("gx", "gy"))
    out_specs = P("lev", "gx", "gy")
    return jax.shard_map(shards, mesh=mesh, in_specs=in_specs, out_specs=out_specs, check_vma=False)
```

```python
import functools

import jax
import jax.numpy as jnp
from jax import lax
from jax.experimental import pallas as pl
from jax.experimental.pallas import tpu as pltpu
from jax.sharding import PartitionSpec as P

SMOOTH = 4
LANES = 128
SUB = 8
SLOT = 24
PER_TILE = 5
PER_SENT = 3
SMALL_RUNG = 1
ROW_BLOCK = 32
F32 = jnp.float32
BF16 = jnp.bfloat16
VMEM_MIB = 1 << 20


def pair_swap(x, axis, parity):
    route = []
    for low in range(parity, lax.axis_size(axis) - 1, 2):
        route += [(low, low + 1), (low + 1, low)]
    return lax.ppermute(x, axis, route)


def call(kernel, grid, in_specs, out_specs, out_shape, scratch=(), flops=1, limit=24):
    return pl.pallas_call(
        kernel,
        grid=grid,
        in_specs=in_specs,
        out_specs=out_specs,
        out_shape=out_shape,
        scratch_shapes=list(scratch),
        compiler_params=pltpu.CompilerParams(vmem_limit_bytes=limit * VMEM_MIB),
        cost_estimate=pl.CostEstimate(flops=flops, bytes_accessed=1 << 20, transcendentals=0),
    )


def smem():
    return pl.BlockSpec(memory_space=pltpu.SMEM)


def whole(*shape):
    return pl.BlockSpec(shape, lambda *_: (0,) * len(shape))


def deal_column(row, size):
    r = lax.broadcasted_iota(jnp.int32, (size, size), 0)
    c = lax.broadcasted_iota(jnp.int32, (size, size), 1)
    return jnp.sum(jnp.where(r == c, row, 0.0), axis=1, keepdims=True)


def share_columns(rows, size, total):
    rows = [row[...].astype(F32).reshape(1, size) for row in rows]
    begins, inside, thick = (deal_column(row, size) for row in rows)
    parent = lax.broadcasted_iota(jnp.int32, (size, LANES), 1).astype(F32)
    raw = jnp.where(parent == begins, inside * thick, 0.0)
    upper = jnp.minimum(begins + 1.0, total - 1.0)
    raw = raw + jnp.where(parent == upper, (1.0 - inside) * thick, 0.0)
    sums = jnp.where(parent < total, jnp.sum(raw, axis=0, keepdims=True), 1.0)
    normed = (raw / sums).astype(BF16).astype(F32)
    low = jnp.sum(jnp.where(parent == begins, normed, 0.0), axis=1, keepdims=True)
    high = jnp.sum(jnp.where(parent == begins + 1.0, normed, 0.0), axis=1, keepdims=True)
    return low, high


def remap_kernel(
    count, total, info, begins, levels, inside, thick, child, own, part, acc, low, high
):
    children, parents = child.shape[0], own.shape[0]
    size, width = low.shape

    @pl.when(pl.program_id(0) == 0)
    def _():
        below, above = share_columns((levels, inside, thick), size, total)
        low[...] = jnp.broadcast_to(below, low.shape)
        high[...] = jnp.broadcast_to(above, high.shape)

    slab = info[7]
    origin = slab * children
    trash = parents + count
    first = begins[origin] - slab * parents
    last = begins[origin + children - 1] - slab * parents

    def clear(p, carry):
        acc[p] = jnp.zeros(acc.shape[1:], F32)
        return carry

    lax.fori_loop(0, jnp.maximum(first, 0), clear, 0)
    untouched = jnp.where(slab == 0, last + 2, parents)
    end = parents + jnp.where(slab == 0, count, jnp.clip(first + count, 0, count))
    lax.fori_loop(untouched, end, clear, 0)

    def step(k, state):
        here, above = state
        level = begins[origin + k]
        rose = level != begins[jnp.maximum(origin + k - 1, 0)]
        value = child[k].astype(F32)
        here = jnp.where(rose, above, here) + low[pl.ds(origin + k, 1), :] * value
        above = jnp.where(rose, 0.0, above) + high[pl.ds(origin + k, 1), :] * value
        place = level - slab * parents
        place = jnp.where(place >= 0, place, parents + count + place)
        acc[jnp.clip(place, 0, trash)] = here
        return here, above

    zero = jnp.zeros(acc.shape[1:], F32)
    here, above = lax.fori_loop(0, children, step, (zero, zero), unroll=4)
    acc[jnp.where(slab == 0, jnp.clip(last + 1, 0, trash), trash)] = above

    def keep(p, carry):
        own[p] = acc[p].astype(BF16)
        return carry

    lax.fori_loop(0, parents, keep, 0, unroll=5)

    def pass_on(j, carry):
        part[j] = acc[parents + j].astype(BF16)
        return carry

    lax.fori_loop(0, count, pass_on, 0)


def blend_kernel(group, own, par, mask, field, old, sems):
    steps = own.shape[0] // group

    def copy(i):
        levels = pl.ds(i * group, group)
        return pltpu.make_async_copy(par.at[levels], old.at[levels], sems.at[i])

    for i in range(steps):
        copy(i).start()
    fed = mask[...] != 0

    def step(i, carry):
        copy(i).wait()
        for j in range(group):
            p = i * group + j
            field[p] = jnp.where(fed, own[p].astype(F32), old[p].astype(F32)).astype(BF16)
        return carry

    lax.fori_loop(0, steps, step, 0)


def rows_kernel(count, info, field_t, field_b, mask_t, mask_b, part_t, part_b, even, odd, top, bot):
    parents = field_t.shape[0]
    row = lax.broadcasted_iota(jnp.int32, field_t.shape[1:], 0)
    flip = info[0] == 1
    fed_t, fed_b = mask_t[...] != 0, mask_b[...] != 0

    def copy(p, carry):
        top[p] = field_t[p].astype(F32)
        bot[p] = field_b[p].astype(F32)
        return carry

    lax.fori_loop(0, parents, copy, 0, unroll=9)

    def add_partner(j, carry):
        p = info[2] + j
        top[p] += jnp.where(fed_t, part_t[j].astype(F32), 0.0)
        bot[p] += jnp.where(fed_b, part_b[j].astype(F32), 0.0)
        return carry

    lax.fori_loop(0, count, add_partner, 0)
    for m in range(even.shape[0]):
        p, q = 2 * m, min(2 * m + 1, parents - 1)
        first = jnp.where(row < SMOOTH, top[p], pltpu.roll(top[q], SMOOTH, 0))
        last = jnp.where(row < SMOOTH, pltpu.roll(bot[p], SMOOTH, 0), bot[q])
        even[m] = jnp.where(flip, first, last).astype(BF16)
        odd[m] = jnp.where(flip, last, first).astype(BF16)


def edge_kernel(count, info, field, mask, part, fixed, edge, sent):
    parents = field.shape[0]
    fed = mask[...] != 0

    def fix(j, carry):
        value = field[info[2] + j].astype(F32) + jnp.where(fed, part[j].astype(F32), 0.0)
        fixed[j] = value.astype(BF16)
        return carry

    lax.fori_loop(0, count, fix, 0)

    def load(p):
        value = field[p].astype(F32)
        for start, near in ((0, p < count), (parents - count, p >= parents - count)):
            if near:
                mine = info[2] == start
                value = jnp.where(mine, fixed[p - start].astype(F32), value)
        return value

    edges = make_edges(parents, load)
    for t, tile in enumerate(edges):
        edge[t] = tile.astype(BF16)
    for t, tile in enumerate(make_sent(edges)):
        sent[t] = tile.astype(BF16)


def make_edges(parents, load):
    tiles = []
    for t in range(pl.cdiv(parents, PER_TILE)):
        tile = None
        for j in range(min(PER_TILE, parents - t * PER_TILE)):
            value = load(t * PER_TILE + j)
            lane = lax.broadcasted_iota(jnp.int32, (value.shape[0], LANES), 1)
            both = jnp.where(lane < LANES // 2, value[:, :LANES], value[:, -LANES:])
            both = pltpu.roll(both, (SLOT * j + 8) % LANES, 1)
            tile = both if tile is None else jnp.where(lane >= SLOT * j, both, tile)
        tiles.append(jnp.where(lane % SLOT < 8, tile, pltpu.roll(tile, 8, 1)))
    return tiles


def make_sent(edges):
    tiles = []
    for q in range(pl.cdiv(len(edges), PER_SENT)):
        tile = None
        for u, edge in enumerate(edges[q * PER_SENT : (q + 1) * PER_SENT]):
            lane = lax.broadcasted_iota(jnp.int32, edge.shape, 1) % SLOT - 8 * u
            last = pltpu.roll(edge, (8 * u - 4) % LANES, 1)
            first = pltpu.roll(edge, (8 * u - 12) % LANES, 1)
            both = jnp.where(lane < 4, last, first)
            tile = both if tile is None else jnp.where(lane >= 0, both, tile)
        tiles.append(tile)
    return tiles


def halo_kernel(parents, info, even, odd, sent_core, halo, edge, sent):
    flip = info[0] == 1
    row = lax.broadcasted_iota(jnp.int32, halo.shape[1:], 0)

    def load(p):
        a, b = even[p // 2].astype(F32), odd[p // 2].astype(F32)
        after, before = jnp.where(flip, b, a), jnp.where(flip, a, b)
        if p % 2 == 0:
            before = pltpu.roll(before, SMOOTH, 0)
        else:
            after = pltpu.roll(after, SMOOTH, 0)
        value = jnp.where(row < SMOOTH, after, before)
        halo[p] = value.astype(BF16)
        return value

    edges = make_edges(parents, load)
    for t, tile in enumerate(edges):
        edge[t] = tile.astype(BF16)
    rows = sent_core.shape[1]
    sent[:, :rows, :] = sent_core[...]
    for t, tile in enumerate(make_sent(edges)):
        sent[t, rows:, :] = tile.astype(BF16)


def row_sweep(values, side_sum, scales, keeps):
    count = len(values)
    before = pltpu.roll(values[-1], 1, 0)
    after = pltpu.roll(values[0], SUB - 1, 0)
    out = []
    for i, value in enumerate(values):
        up = values[i - 1] if i > 0 else before
        down = values[i + 1] if i < count - 1 else after
        out.append(keeps[i] * value + scales[i] * ((up + down) + side_sum(i, value)))
    return out


def row_flags(info, count, rows):
    sub = lax.broadcasted_iota(jnp.int32, (SUB, LANES), 0)
    flags = []
    for i in range(count):
        r = (SUB - 1) * count + i - rows
        if r < 0:
            flags.append(None)
            continue
        inside = info[4] if r < SMOOTH else info[3]
        flags.append(jnp.where(sub == SUB - 1, inside.astype(F32), 1.0))
    return flags


def smooth_kernel(count, info, coefs, field, fixed, halo, out, left, right, work, sides, near):
    levels, rows = field.shape[:2]
    deals = left.shape[1] // SUB
    flags = row_flags(info, deals, rows)
    flags = [None if f is None else jnp.concatenate([f, f], axis=1) for f in flags]
    base = pl.program_id(0) * levels

    @pl.when(pl.program_id(0) == 0)
    def _():
        r = lax.broadcasted_iota(jnp.int32, near.shape, 0)
        c = lax.broadcasted_iota(jnp.int32, near.shape, 1)
        near[...] = jnp.where(jnp.abs(r - c) == 1, 1.0, 0.0).astype(BF16)

    weights = []
    for p in range(levels):
        scale = coefs[base + p]
        keep = 1.0 - 4.0 * scale
        weights.append(
            (
                [scale if f is None else scale * f for f in flags],
                [keep if f is None else keep * f for f in flags],
            )
        )
        j = base + p - info[2]
        use_fixed = (j >= 0) & (j < count)
        j = jnp.clip(j, 0, count - 1)
        for ref, cut in ((left, slice(0, LANES)), (right, slice(LANES, 2 * LANES))):
            ref[p, :rows, :] = field[p, :, cut].astype(F32)

            @pl.when(use_fixed)
            def _():
                ref[p, :rows, :] = fixed[j, :, cut].astype(F32)

            ref[p, rows:, :] = halo[p, :, cut].astype(F32)
        for i in range(deals):
            part = slice(SUB * i, SUB * i + SUB)
            work[0, p, part, :LANES] = left[p, pl.ds(i, SUB, stride=deals), :]
            work[0, p, part, LANES:] = right[p, pl.ds(i, SUB, stride=deals), :]
    for s in range(SMOOTH):
        flat = work[s % 2].reshape(levels * deals * SUB, 2 * LANES).astype(BF16)
        side = jnp.dot(flat, near[...], preferred_element_type=F32)
        sides[...] = side.reshape(sides.shape)
        for p in range(levels):
            values = [work[s % 2, p, SUB * i : SUB * i + SUB, :] for i in range(deals)]
            values = row_sweep(
                values, lambda i, _: sides[p, SUB * i : SUB * i + SUB, :], *weights[p]
            )
            for i, value in enumerate(values):
                if s == SMOOTH - 1:
                    left[p, pl.ds(i, SUB, stride=deals), :] = value[:, :LANES]
                    right[p, pl.ds(i, SUB, stride=deals), :] = value[:, LANES:]
                else:
                    work[(s + 1) % 2, p, SUB * i : SUB * i + SUB, :] = value
    for p in range(levels):
        out[p, :, :LANES] = left[p, :rows, :].astype(BF16)
        out[p, :, LANES:] = right[p, :rows, :].astype(BF16)


def seam_kernel(info, coefs, even, odd, core, edge, main, out, tiles, work, done, sems):
    total = tiles.shape[0]
    rows = core.shape[1]
    count = tiles.shape[1] // SUB
    step = pl.program_id(0)

    @pl.when(step == 0)
    def _():
        flip = info[1] == 1
        flags = row_flags(info, count, rows)
        slot = lax.broadcasted_iota(jnp.int32, tiles.shape[1:], 1) % SLOT
        for q in range(even.shape[0]):
            a, b = even[q].astype(F32), odd[q].astype(F32)
            after, before = jnp.where(flip, b, a), jnp.where(flip, a, b)
            for u in range(min(PER_SENT, total - q * PER_SENT)):
                t = q * PER_SENT + u
                own = jnp.concatenate([core[t].astype(F32), edge[t].astype(F32)], axis=0)
                right = pltpu.roll(after, (4 - 8 * u) % LANES, 1)
                left = pltpu.roll(before, (12 - 8 * u) % LANES, 1)
                tile = jnp.where(slot < 12, right, left)
                tiles[t] = jnp.where((slot >= 8) & (slot < 16), tile, own)
        for t in range(total):
            for i in range(count):
                work[0, t, i] = tiles[t, pl.ds(i, SUB, stride=count), :]
        for s in range(SMOOTH):
            for t in range(total):
                scale = coefs[0, t]
                keep = coefs[1, t]
                scales = [scale if f is None else scale * f for f in flags]
                keeps = [keep if f is None else keep * f for f in flags]
                values = [work[s % 2, t, i] for i in range(count)]
                new = row_sweep(
                    values,
                    lambda _, x: pltpu.roll(x, 1, 1) + pltpu.roll(x, LANES - 1, 1),
                    scales,
                    keeps,
                )
                for i in range(count):
                    if s < SMOOTH - 1:
                        work[(s + 1) % 2, t, i] = new[i]
                    else:
                        tiles[t, pl.ds(i, SUB, stride=count), :] = new[i]

    seam = tiles[step, :rows, :]
    lane = lax.broadcasted_iota(jnp.int32, seam.shape, 1)
    seam = jnp.where(lane % SLOT < 8, seam, pltpu.roll(seam, LANES - 8, 1))
    group = main.shape[0]
    for j in range(group):
        both = pltpu.roll(seam, (120 - SLOT * j) % LANES, 1)
        a, b = main[j, :, :LANES].astype(F32), main[j, :, LANES:].astype(F32)
        p = step * group + j
        done[p, :, :LANES] = jnp.where(lane < SMOOTH, both, a).astype(BF16)
        done[p, :, LANES:] = jnp.where(lane >= LANES - SMOOTH, both, b).astype(BF16)

    def copy(i):
        levels = pl.ds(i * group, group)
        return pltpu.make_async_copy(done.at[levels], out.at[levels], sems.at[i])

    copy(step).start()

    @pl.when(step == total - 1)
    def _():
        for i in range(total):
            copy(i).wait()


def device_facts(start):
    slab, gx, gy = lax.axis_index("lev"), lax.axis_index("gx"), lax.axis_index("gy")
    facts = [
        gx % 2,
        gy % 2,
        start,
        gx > 0,
        gx < lax.axis_size("gx") - 1,
        gy > 0,
        gy < lax.axis_size("gy") - 1,
        slab,
    ]
    return jnp.stack([jnp.asarray(fact, jnp.int32) for fact in facts])


def feed_back(count, child, parent, inside, thick, level_map, smooth_coef, mask):
    children, rows, columns = child.shape
    parents = parent.shape[0]
    total = parents * lax.axis_size("lev")
    size = level_map.shape[0]
    slab = lax.axis_index("lev")
    info = device_facts(jnp.where(slab == 0, parents - count, 0))
    block = ROW_BLOCK
    own, part = call(
        functools.partial(remap_kernel, count, total),
        (rows // block,),
        [
            smem(), smem(), whole(size), whole(size), whole(size),
            pl.BlockSpec((children, block, columns), lambda i: (0, i, 0)),
        ],
        [
            pl.BlockSpec((parents, block, columns), lambda i: (0, i, 0)),
            pl.BlockSpec((count, block, columns), lambda i: (0, i, 0)),
        ],
        [
            jax.ShapeDtypeStruct((parents, rows, columns), BF16),
            jax.ShapeDtypeStruct((count, rows, columns), BF16),
        ],
        [pltpu.VMEM((parents + count + 1, block, columns), F32)]
        + [pltpu.VMEM((size, columns), F32)] * 2,
    )(info, level_map, level_map, inside, thick, child)
    part = pair_swap(part, "lev", 0)
    group = PER_TILE
    field = call(
        functools.partial(blend_kernel, group),
        (1,),
        [whole(parents, rows, columns), pl.BlockSpec(memory_space=pltpu.HBM), whole(rows, columns)],
        whole(parents, rows, columns),
        jax.ShapeDtypeStruct((parents, rows, columns), BF16),
        [
            pltpu.VMEM((parents, rows, columns), BF16),
            pltpu.SemaphoreType.DMA((parents // group,)),
        ],
        flops=1 << 34,
    )(own, parent, mask)

    ends = rows // SUB - 1

    def two(lead):
        return [
            pl.BlockSpec((lead, SUB, columns), lambda i: (0, 0, 0)),
            pl.BlockSpec((lead, SUB, columns), lambda i: (0, ends, 0)),
        ]

    packed = pl.cdiv(parents, 2)
    strip = jax.ShapeDtypeStruct((packed, SUB, columns), BF16)
    row_even, row_odd = call(
        functools.partial(rows_kernel, count),
        (1,),
        [
            smem(),
            *two(parents),
            pl.BlockSpec((SUB, columns), lambda i: (0, 0)),
            pl.BlockSpec((SUB, columns), lambda i: (ends, 0)),
            *two(count),
        ],
        [whole(packed, SUB, columns)] * 2,
        [strip, strip],
        [pltpu.VMEM((parents, SUB, columns), F32)] * 2,
    )(info, field, field, mask, mask, part, part)
    row_even = pair_swap(row_even, "gx", 0)
    row_odd = pair_swap(row_odd, "gx", 1)

    seams = pl.cdiv(parents, PER_TILE)
    sents = pl.cdiv(seams, PER_SENT)
    fixed, edge_core, sent_core = call(
        functools.partial(edge_kernel, count),
        (rows // block,),
        [
            smem(),
            pl.BlockSpec((parents, block, columns), lambda i: (0, i, 0)),
            pl.BlockSpec((block, columns), lambda i: (i, 0)),
            pl.BlockSpec((count, block, columns), lambda i: (0, i, 0)),
        ],
        [
            pl.BlockSpec((count, block, columns), lambda i: (0, i, 0)),
            pl.BlockSpec((seams, block, LANES), lambda i: (0, i, 0)),
            pl.BlockSpec((sents, block, LANES), lambda i: (0, i, 0)),
        ],
        [
            jax.ShapeDtypeStruct((count, rows, columns), BF16),
            jax.ShapeDtypeStruct((seams, rows, LANES), BF16),
            jax.ShapeDtypeStruct((sents, rows, LANES), BF16),
        ],
        flops=1 << 34,
    )(info, field, mask, part)

    extended = rows + SUB
    halo, edge_halo, sent = call(
        functools.partial(halo_kernel, parents),
        (1,),
        [smem(), whole(packed, SUB, columns), whole(packed, SUB, columns), whole(sents, rows, LANES)],
        [whole(parents, SUB, columns), whole(seams, SUB, LANES), whole(sents, extended, LANES)],
        [
            jax.ShapeDtypeStruct((parents, SUB, columns), BF16),
            jax.ShapeDtypeStruct((seams, SUB, LANES), BF16),
            jax.ShapeDtypeStruct((sents, extended, LANES), BF16),
        ],
    )(info, row_even, row_odd, sent_core)
    column_even = pair_swap(sent, "gy", 0)
    column_odd = pair_swap(sent, "gy", 1)

    group = PER_TILE
    main = call(
        functools.partial(smooth_kernel, count),
        (parents // group,),
        [
            smem(), smem(),
            pl.BlockSpec((group, rows, columns), lambda i: (i, 0, 0)),
            whole(count, rows, columns),
            pl.BlockSpec((group, SUB, columns), lambda i: (i, 0, 0)),
        ],
        pl.BlockSpec((group, rows, columns), lambda i: (i, 0, 0)),
        jax.ShapeDtypeStruct((parents, rows, columns), BF16),
        [pltpu.VMEM((group, extended, LANES), F32)] * 2
        + [
            pltpu.VMEM((2, group, extended, columns), F32),
            pltpu.VMEM((group, extended, columns), F32),
            pltpu.VMEM((columns, columns), BF16),
        ],
        flops=1 << 34,
    )(info, smooth_coef, field, fixed, halo)

    return finish(info, smooth_coef, column_even, column_odd, edge_core, edge_halo, main)


def finish(info, smooth_coef, column_even, column_odd, edge_core, edge_halo, main):
    parents, rows, columns = main.shape
    seams, extended = edge_core.shape[0], column_even.shape[1]
    sents, group = column_even.shape[0], PER_TILE
    gy = lax.axis_index("gy")
    lane = jnp.arange(LANES, dtype=jnp.int32)
    place_in_slot = lane % SLOT
    inside = lane < SLOT * PER_TILE
    after = (place_in_slot >= 8) & (place_in_slot < 12)
    before = (place_in_slot >= 12) & (place_in_slot < 16)
    inside &= ~after | (gy < lax.axis_size("gy") - 1)
    inside &= ~before | (gy > 0)
    by_tile = jnp.repeat(smooth_coef.reshape(seams, PER_TILE), SLOT, axis=1)
    by_tile = jnp.pad(by_tile, ((0, 0), (0, LANES - SLOT * PER_TILE)))
    lane_coefs = jnp.where(inside, jnp.stack([by_tile, 1.0 - 4.0 * by_tile]), 0.0)
    lane_coefs = jnp.broadcast_to(lane_coefs[:, :, None, :], (2, seams, SUB, LANES))
    return call(
        seam_kernel,
        (seams,),
        [
            smem(),
            whole(2, seams, SUB, LANES),
            whole(sents, extended, LANES),
            whole(sents, extended, LANES),
            whole(seams, rows, LANES),
            whole(seams, SUB, LANES),
            pl.BlockSpec((group, rows, columns), lambda i: (i, 0, 0)),
        ],
        pl.BlockSpec(memory_space=pltpu.HBM),
        pltpu.HBM((parents, rows, columns), BF16),
        [
            pltpu.VMEM((seams, extended, LANES), F32),
            pltpu.VMEM((2, seams, extended // SUB, SUB, LANES), F32),
            pltpu.VMEM((parents, rows, columns), BF16),
            pltpu.SemaphoreType.DMA((seams,)),
        ],
    )(info, lane_coefs, column_even, column_odd, edge_core, edge_halo, main)


def shards(child_field, parent_old, level_map, intersection, thickness, smooth_coef, nest_mask):
    children, parents = child_field.shape[0], parent_old.shape[0]
    most = children - parents + 1
    ends = level_map[children - 1 : children + 1]
    crossing = jnp.max(ends * jnp.array([1, -1]) + jnp.array([2 - parents, parents]))

    def run(count):
        return lambda: feed_back(
            count, child_field, parent_old, intersection, thickness, level_map, smooth_coef, nest_mask
        )

    return lax.cond(crossing <= SMALL_RUNG, run(SMALL_RUNG), run(most))


def solution(mesh):
    in_specs = (P("lev", "gx", "gy"), P("lev", "gx", "gy"), P(), P(), P(), P("lev"), P("gx", "gy"))
    out_specs = P("lev", "gx", "gy")
    return jax.shard_map(shards, mesh=mesh, in_specs=in_specs, out_specs=out_specs, check_vma=False)
```

```python
import functools

import jax
import jax.numpy as jnp
from jax import lax
from jax.experimental import pallas as pl
from jax.experimental.pallas import tpu as pltpu
from jax.sharding import PartitionSpec as P

SMOOTH = 4
LANES = 128
SUB = 8
SLOT = 24
PER_TILE = 5
PER_SENT = 3
SMALL_RUNG = 1
ROW_BLOCK = 32
F32 = jnp.float32
BF16 = jnp.bfloat16
VMEM_MIB = 1 << 20


def pair_swap(x, axis, parity):
    route = []
    for low in range(parity, lax.axis_size(axis) - 1, 2):
        route += [(low, low + 1), (low + 1, low)]
    return lax.ppermute(x, axis, route)


def call(kernel, grid, in_specs, out_specs, out_shape, scratch=(), flops=1, limit=24):
    return pl.pallas_call(
        kernel,
        grid=grid,
        in_specs=in_specs,
        out_specs=out_specs,
        out_shape=out_shape,
        scratch_shapes=list(scratch),
        compiler_params=pltpu.CompilerParams(vmem_limit_bytes=limit * VMEM_MIB),
        cost_estimate=pl.CostEstimate(flops=flops, bytes_accessed=1 << 20, transcendentals=0),
    )


def smem():
    return pl.BlockSpec(memory_space=pltpu.SMEM)


def whole(*shape):
    return pl.BlockSpec(shape, lambda *_: (0,) * len(shape))


def deal_column(row, size):
    r = lax.broadcasted_iota(jnp.int32, (size, size), 0)
    c = lax.broadcasted_iota(jnp.int32, (size, size), 1)
    return jnp.sum(jnp.where(r == c, row, 0.0), axis=1, keepdims=True)


def share_columns(rows, size, total):
    rows = [row[...].astype(F32).reshape(1, size) for row in rows]
    begins, inside, thick = (deal_column(row, size) for row in rows)
    parent = lax.broadcasted_iota(jnp.int32, (size, LANES), 1).astype(F32)
    raw = jnp.where(parent == begins, inside * thick, 0.0)
    upper = jnp.minimum(begins + 1.0, total - 1.0)
    raw = raw + jnp.where(parent == upper, (1.0 - inside) * thick, 0.0)
    sums = jnp.where(parent < total, jnp.sum(raw, axis=0, keepdims=True), 1.0)
    normed = (raw / sums).astype(BF16).astype(F32)
    low = jnp.sum(jnp.where(parent == begins, normed, 0.0), axis=1, keepdims=True)
    high = jnp.sum(jnp.where(parent == begins + 1.0, normed, 0.0), axis=1, keepdims=True)
    return low, high


def remap_kernel(
    count, total, info, begins, levels, inside, thick, child, own, part, acc, low, high, held, sems
):
    children, parents = child.shape[0], own.shape[0]
    size, width = low.shape

    block = acc.shape[1]
    chunks = held.shape[1] // block

    def copy(i):
        rows = pl.ds(pl.multiple_of(i * block, block), block)
        return pltpu.make_async_copy(child.at[:, rows, :], held.at[:, rows, :], sems.at[i])

    for i in range(chunks):
        copy(i).start()
    below, above = share_columns((levels, inside, thick), size, total)
    low[...] = jnp.broadcast_to(below, low.shape)
    high[...] = jnp.broadcast_to(above, high.shape)
    slab = info[7]
    origin = slab * children
    trash = parents + count
    first = begins[origin] - slab * parents
    last = begins[origin + children - 1] - slab * parents

    def clear(p, carry):
        acc[p] = jnp.zeros(acc.shape[1:], F32)
        return carry

    lax.fori_loop(0, jnp.maximum(first, 0), clear, 0)
    untouched = jnp.where(slab == 0, last + 2, parents)
    end = parents + jnp.where(slab == 0, count, jnp.clip(first + count, 0, count))
    lax.fori_loop(untouched, end, clear, 0)

    def chunk(i, carry):
        copy(i).wait()
        rows = pl.ds(pl.multiple_of(i * block, block), block)

        def step(k, state):
            here, above = state
            level = begins[origin + k]
            rose = level != begins[jnp.maximum(origin + k - 1, 0)]
            value = held[k, rows, :].astype(F32)
            here = jnp.where(rose, above, here) + low[pl.ds(origin + k, 1), :] * value
            above = jnp.where(rose, 0.0, above) + high[pl.ds(origin + k, 1), :] * value
            place = level - slab * parents
            place = jnp.where(place >= 0, place, parents + count + place)
            acc[jnp.clip(place, 0, trash)] = here
            return here, above

        zero = jnp.zeros(acc.shape[1:], F32)
        here, above = lax.fori_loop(0, children, step, (zero, zero), unroll=4)
        acc[jnp.where(slab == 0, jnp.clip(last + 1, 0, trash), trash)] = above

        def keep(p, carry):
            own[p, rows, :] = acc[p].astype(BF16)
            return carry

        lax.fori_loop(0, parents, keep, 0, unroll=5)

        def pass_on(j, carry):
            part[j, rows, :] = acc[parents + j].astype(BF16)
            return carry

        lax.fori_loop(0, count, pass_on, 0)
        return carry

    lax.fori_loop(0, chunks, chunk, 0)


def blend_kernel(group, own, par, mask, field, old, sems):
    steps = own.shape[0] // group

    def copy(i):
        levels = pl.ds(i * group, group)
        return pltpu.make_async_copy(par.at[levels], old.at[levels], sems.at[i])

    for i in range(steps):
        copy(i).start()
    fed = mask[...] != 0

    def step(i, carry):
        copy(i).wait()
        for j in range(group):
            p = i * group + j
            field[p] = jnp.where(fed, own[p].astype(F32), old[p].astype(F32)).astype(BF16)
        return carry

    lax.fori_loop(0, steps, step, 0)


def rows_kernel(count, info, field_t, field_b, mask_t, mask_b, part_t, part_b, even, odd, top, bot):
    parents = field_t.shape[0]
    row = lax.broadcasted_iota(jnp.int32, field_t.shape[1:], 0)
    flip = info[0] == 1
    fed_t, fed_b = mask_t[...] != 0, mask_b[...] != 0

    def copy(p, carry):
        top[p] = field_t[p].astype(F32)
        bot[p] = field_b[p].astype(F32)
        return carry

    lax.fori_loop(0, parents, copy, 0, unroll=9)

    def add_partner(j, carry):
        p = info[2] + j
        top[p] += jnp.where(fed_t, part_t[j].astype(F32), 0.0)
        bot[p] += jnp.where(fed_b, part_b[j].astype(F32), 0.0)
        return carry

    lax.fori_loop(0, count, add_partner, 0)
    for m in range(even.shape[0]):
        p, q = 2 * m, min(2 * m + 1, parents - 1)
        first = jnp.where(row < SMOOTH, top[p], pltpu.roll(top[q], SMOOTH, 0))
        last = jnp.where(row < SMOOTH, pltpu.roll(bot[p], SMOOTH, 0), bot[q])
        even[m] = jnp.where(flip, first, last).astype(BF16)
        odd[m] = jnp.where(flip, last, first).astype(BF16)


def edge_kernel(count, info, field, mask, part, fixed, edge, sent):
    parents = field.shape[0]
    fed = mask[...] != 0

    def fix(j, carry):
        value = field[info[2] + j].astype(F32) + jnp.where(fed, part[j].astype(F32), 0.0)
        fixed[j] = value.astype(BF16)
        return carry

    lax.fori_loop(0, count, fix, 0)

    def load(p):
        value = field[p].astype(F32)
        for start, near in ((0, p < count), (parents - count, p >= parents - count)):
            if near:
                mine = info[2] == start
                value = jnp.where(mine, fixed[p - start].astype(F32), value)
        return value

    edges = make_edges(parents, load)
    for t, tile in enumerate(edges):
        edge[t] = tile.astype(BF16)
    for t, tile in enumerate(make_sent(edges)):
        sent[t] = tile.astype(BF16)


def make_edges(parents, load):
    tiles = []
    for t in range(pl.cdiv(parents, PER_TILE)):
        tile = None
        for j in range(min(PER_TILE, parents - t * PER_TILE)):
            value = load(t * PER_TILE + j)
            lane = lax.broadcasted_iota(jnp.int32, (value.shape[0], LANES), 1)
            both = jnp.where(lane < LANES // 2, value[:, :LANES], value[:, -LANES:])
            both = pltpu.roll(both, (SLOT * j + 8) % LANES, 1)
            tile = both if tile is None else jnp.where(lane >= SLOT * j, both, tile)
        tiles.append(jnp.where(lane % SLOT < 8, tile, pltpu.roll(tile, 8, 1)))
    return tiles


def make_sent(edges):
    tiles = []
    for q in range(pl.cdiv(len(edges), PER_SENT)):
        tile = None
        for u, edge in enumerate(edges[q * PER_SENT : (q + 1) * PER_SENT]):
            lane = lax.broadcasted_iota(jnp.int32, edge.shape, 1) % SLOT - 8 * u
            last = pltpu.roll(edge, (8 * u - 4) % LANES, 1)
            first = pltpu.roll(edge, (8 * u - 12) % LANES, 1)
            both = jnp.where(lane < 4, last, first)
            tile = both if tile is None else jnp.where(lane >= 0, both, tile)
        tiles.append(tile)
    return tiles


def halo_kernel(parents, info, even, odd, sent_core, halo, edge, sent):
    flip = info[0] == 1
    row = lax.broadcasted_iota(jnp.int32, halo.shape[1:], 0)

    def load(p):
        a, b = even[p // 2].astype(F32), odd[p // 2].astype(F32)
        after, before = jnp.where(flip, b, a), jnp.where(flip, a, b)
        if p % 2 == 0:
            before = pltpu.roll(before, SMOOTH, 0)
        else:
            after = pltpu.roll(after, SMOOTH, 0)
        value = jnp.where(row < SMOOTH, after, before)
        halo[p] = value.astype(BF16)
        return value

    edges = make_edges(parents, load)
    for t, tile in enumerate(edges):
        edge[t] = tile.astype(BF16)
    rows = sent_core.shape[1]
    sent[:, :rows, :] = sent_core[...]
    for t, tile in enumerate(make_sent(edges)):
        sent[t, rows:, :] = tile.astype(BF16)


def row_sweep(values, side_sum, scales, keeps):
    count = len(values)
    before = pltpu.roll(values[-1], 1, 0)
    after = pltpu.roll(values[0], SUB - 1, 0)
    out = []
    for i, value in enumerate(values):
        up = values[i - 1] if i > 0 else before
        down = values[i + 1] if i < count - 1 else after
        out.append(keeps[i] * value + scales[i] * ((up + down) + side_sum(i, value)))
    return out


def row_flags(info, count, rows):
    sub = lax.broadcasted_iota(jnp.int32, (SUB, LANES), 0)
    flags = []
    for i in range(count):
        r = (SUB - 1) * count + i - rows
        if r < 0:
            flags.append(None)
            continue
        inside = info[4] if r < SMOOTH else info[3]
        flags.append(jnp.where(sub == SUB - 1, inside.astype(F32), 1.0))
    return flags


def smooth_kernel(count, info, coefs, field, fixed, halo, out, left, right, work, sides, near):
    levels, rows = left.shape[0], field.shape[1]
    deals = left.shape[1] // SUB
    flags = row_flags(info, deals, rows)
    flags = [None if f is None else jnp.concatenate([f, f], axis=1) for f in flags]
    r = lax.broadcasted_iota(jnp.int32, near.shape, 0)
    c = lax.broadcasted_iota(jnp.int32, near.shape, 1)
    near[...] = jnp.where(jnp.abs(r - c) == 1, 1.0, 0.0).astype(BF16)

    def group(g, carry):
        base = g * levels
        weights = []
        for p in range(levels):
            scale = coefs[base + p]
            keep = 1.0 - 4.0 * scale
            weights.append(
                (
                    [scale if f is None else scale * f for f in flags],
                    [keep if f is None else keep * f for f in flags],
                )
            )
            j = base + p - info[2]
            use_fixed = (j >= 0) & (j < count)
            j = jnp.clip(j, 0, count - 1)
            for ref, cut in ((left, slice(0, LANES)), (right, slice(LANES, 2 * LANES))):
                ref[p, :rows, :] = field[base + p, :, cut].astype(F32)

                @pl.when(use_fixed)
                def _():
                    ref[p, :rows, :] = fixed[j, :, cut].astype(F32)

                ref[p, rows:, :] = halo[base + p, :, cut].astype(F32)
            for i in range(deals):
                part = slice(SUB * i, SUB * i + SUB)
                work[0, p, part, :LANES] = left[p, pl.ds(i, SUB, stride=deals), :]
                work[0, p, part, LANES:] = right[p, pl.ds(i, SUB, stride=deals), :]
        for s in range(SMOOTH):
            flat = work[s % 2].reshape(levels * deals * SUB, 2 * LANES).astype(BF16)
            side = jnp.dot(flat, near[...], preferred_element_type=F32)
            sides[...] = side.reshape(sides.shape)
            for p in range(levels):
                values = [work[s % 2, p, SUB * i : SUB * i + SUB, :] for i in range(deals)]
                values = row_sweep(
                    values, lambda i, _: sides[p, SUB * i : SUB * i + SUB, :], *weights[p]
                )
                for i, value in enumerate(values):
                    if s == SMOOTH - 1:
                        left[p, pl.ds(i, SUB, stride=deals), :] = value[:, :LANES]
                        right[p, pl.ds(i, SUB, stride=deals), :] = value[:, LANES:]
                    else:
                        work[(s + 1) % 2, p, SUB * i : SUB * i + SUB, :] = value
        for p in range(levels):
            out[base + p, :, :LANES] = left[p, :rows, :].astype(BF16)
            out[base + p, :, LANES:] = right[p, :rows, :].astype(BF16)
        return carry

    lax.fori_loop(0, field.shape[0] // levels, group, 0)


def seam_kernel(info, coefs, even, odd, core, edge, main, out, tiles, work, done, sems):
    total = tiles.shape[0]
    rows = core.shape[1]
    count = tiles.shape[1] // SUB
    flip = info[1] == 1
    flags = row_flags(info, count, rows)
    slot = lax.broadcasted_iota(jnp.int32, tiles.shape[1:], 1) % SLOT
    for q in range(even.shape[0]):
        a, b = even[q].astype(F32), odd[q].astype(F32)
        after, before = jnp.where(flip, b, a), jnp.where(flip, a, b)
        for u in range(min(PER_SENT, total - q * PER_SENT)):
            t = q * PER_SENT + u
            own = jnp.concatenate([core[t].astype(F32), edge[t].astype(F32)], axis=0)
            right = pltpu.roll(after, (4 - 8 * u) % LANES, 1)
            left = pltpu.roll(before, (12 - 8 * u) % LANES, 1)
            tile = jnp.where(slot < 12, right, left)
            tiles[t] = jnp.where((slot >= 8) & (slot < 16), tile, own)
    for t in range(total):
        for i in range(count):
            work[0, t, i] = tiles[t, pl.ds(i, SUB, stride=count), :]
    for s in range(SMOOTH):
        for t in range(total):
            scale = coefs[0, t]
            keep = coefs[1, t]
            scales = [scale if f is None else scale * f for f in flags]
            keeps = [keep if f is None else keep * f for f in flags]
            values = [work[s % 2, t, i] for i in range(count)]
            new = row_sweep(
                values,
                lambda _, x: pltpu.roll(x, 1, 1) + pltpu.roll(x, LANES - 1, 1),
                scales,
                keeps,
            )
            for i in range(count):
                if s < SMOOTH - 1:
                    work[(s + 1) % 2, t, i] = new[i]
                else:
                    tiles[t, pl.ds(i, SUB, stride=count), :] = new[i]

    group = main.shape[0] // total

    def copy(i):
        levels = pl.ds(i * group, group)
        return pltpu.make_async_copy(done.at[levels], out.at[levels], sems.at[i])

    def step(i, carry):
        seam = tiles[i, :rows, :]
        lane = lax.broadcasted_iota(jnp.int32, seam.shape, 1)
        seam = jnp.where(lane % SLOT < 8, seam, pltpu.roll(seam, LANES - 8, 1))
        for j in range(group):
            both = pltpu.roll(seam, (120 - SLOT * j) % LANES, 1)
            p = i * group + j
            a, b = main[p, :, :LANES].astype(F32), main[p, :, LANES:].astype(F32)
            done[p, :, :LANES] = jnp.where(lane < SMOOTH, both, a).astype(BF16)
            done[p, :, LANES:] = jnp.where(lane >= LANES - SMOOTH, both, b).astype(BF16)
        copy(i).start()
        return carry

    lax.fori_loop(0, total, step, 0)
    for i in range(total):
        copy(i).wait()


def device_facts(start):
    slab, gx, gy = lax.axis_index("lev"), lax.axis_index("gx"), lax.axis_index("gy")
    facts = [
        gx % 2,
        gy % 2,
        start,
        gx > 0,
        gx < lax.axis_size("gx") - 1,
        gy > 0,
        gy < lax.axis_size("gy") - 1,
        slab,
    ]
    return jnp.stack([jnp.asarray(fact, jnp.int32) for fact in facts])


def feed_back(count, child, parent, inside, thick, level_map, smooth_coef, mask):
    children, rows, columns = child.shape
    parents = parent.shape[0]
    total = parents * lax.axis_size("lev")
    size = level_map.shape[0]
    slab = lax.axis_index("lev")
    info = device_facts(jnp.where(slab == 0, parents - count, 0))
    block = ROW_BLOCK
    own, part = call(
        functools.partial(remap_kernel, count, total),
        (1,),
        [
            smem(), smem(), whole(size), whole(size), whole(size),
            pl.BlockSpec(memory_space=pltpu.HBM),
        ],
        [whole(parents, rows, columns), whole(count, rows, columns)],
        [
            jax.ShapeDtypeStruct((parents, rows, columns), BF16),
            jax.ShapeDtypeStruct((count, rows, columns), BF16),
        ],
        [
            pltpu.VMEM((parents + count + 1, block, columns), F32),
            pltpu.VMEM((size, columns), F32),
            pltpu.VMEM((size, columns), F32),
            pltpu.VMEM((children, rows, columns), BF16),
            pltpu.SemaphoreType.DMA((rows // block,)),
        ],
    )(info, level_map, level_map, inside, thick, child)
    part = pair_swap(part, "lev", 0)
    group = PER_TILE
    field = call(
        functools.partial(blend_kernel, group),
        (1,),
        [whole(parents, rows, columns), pl.BlockSpec(memory_space=pltpu.HBM), whole(rows, columns)],
        whole(parents, rows, columns),
        jax.ShapeDtypeStruct((parents, rows, columns), BF16),
        [
            pltpu.VMEM((parents, rows, columns), BF16),
            pltpu.SemaphoreType.DMA((parents // group,)),
        ],
        flops=1 << 34,
    )(own, parent, mask)

    ends = rows // SUB - 1

    def two(lead):
        return [
            pl.BlockSpec((lead, SUB, columns), lambda i: (0, 0, 0)),
            pl.BlockSpec((lead, SUB, columns), lambda i: (0, ends, 0)),
        ]

    packed = pl.cdiv(parents, 2)
    strip = jax.ShapeDtypeStruct((packed, SUB, columns), BF16)
    row_even, row_odd = call(
        functools.partial(rows_kernel, count),
        (1,),
        [
            smem(),
            *two(parents),
            pl.BlockSpec((SUB, columns), lambda i: (0, 0)),
            pl.BlockSpec((SUB, columns), lambda i: (ends, 0)),
            *two(count),
        ],
        [whole(packed, SUB, columns)] * 2,
        [strip, strip],
        [pltpu.VMEM((parents, SUB, columns), F32)] * 2,
    )(info, field, field, mask, mask, part, part)
    row_even = pair_swap(row_even, "gx", 0)
    row_odd = pair_swap(row_odd, "gx", 1)

    seams = pl.cdiv(parents, PER_TILE)
    sents = pl.cdiv(seams, PER_SENT)
    fixed, edge_core, sent_core = call(
        functools.partial(edge_kernel, count),
        (rows // block,),
        [
            smem(),
            pl.BlockSpec((parents, block, columns), lambda i: (0, i, 0)),
            pl.BlockSpec((block, columns), lambda i: (i, 0)),
            pl.BlockSpec((count, block, columns), lambda i: (0, i, 0)),
        ],
        [
            pl.BlockSpec((count, block, columns), lambda i: (0, i, 0)),
            pl.BlockSpec((seams, block, LANES), lambda i: (0, i, 0)),
            pl.BlockSpec((sents, block, LANES), lambda i: (0, i, 0)),
        ],
        [
            jax.ShapeDtypeStruct((count, rows, columns), BF16),
            jax.ShapeDtypeStruct((seams, rows, LANES), BF16),
            jax.ShapeDtypeStruct((sents, rows, LANES), BF16),
        ],
        flops=1 << 34,
    )(info, field, mask, part)

    extended = rows + SUB
    halo, edge_halo, sent = call(
        functools.partial(halo_kernel, parents),
        (1,),
        [smem(), whole(packed, SUB, columns), whole(packed, SUB, columns), whole(sents, rows, LANES)],
        [whole(parents, SUB, columns), whole(seams, SUB, LANES), whole(sents, extended, LANES)],
        [
            jax.ShapeDtypeStruct((parents, SUB, columns), BF16),
            jax.ShapeDtypeStruct((seams, SUB, LANES), BF16),
            jax.ShapeDtypeStruct((sents, extended, LANES), BF16),
        ],
    )(info, row_even, row_odd, sent_core)
    column_even = pair_swap(sent, "gy", 0)
    column_odd = pair_swap(sent, "gy", 1)

    group = PER_TILE
    main = call(
        functools.partial(smooth_kernel, count),
        (1,),
        [
            smem(), smem(),
            whole(parents, rows, columns),
            whole(count, rows, columns),
            whole(parents, SUB, columns),
        ],
        whole(parents, rows, columns),
        jax.ShapeDtypeStruct((parents, rows, columns), BF16),
        [pltpu.VMEM((group, extended, LANES), F32)] * 2
        + [
            pltpu.VMEM((2, group, extended, columns), F32),
            pltpu.VMEM((group, extended, columns), F32),
            pltpu.VMEM((columns, columns), BF16),
        ],
        flops=1 << 34,
    )(info, smooth_coef, field, fixed, halo)

    return finish(info, smooth_coef, column_even, column_odd, edge_core, edge_halo, main)


def finish(info, smooth_coef, column_even, column_odd, edge_core, edge_halo, main):
    parents, rows, columns = main.shape
    seams, extended = edge_core.shape[0], column_even.shape[1]
    sents, group = column_even.shape[0], PER_TILE
    gy = lax.axis_index("gy")
    lane = jnp.arange(LANES, dtype=jnp.int32)
    place_in_slot = lane % SLOT
    inside = lane < SLOT * PER_TILE
    after = (place_in_slot >= 8) & (place_in_slot < 12)
    before = (place_in_slot >= 12) & (place_in_slot < 16)
    inside &= ~after | (gy < lax.axis_size("gy") - 1)
    inside &= ~before | (gy > 0)
    by_tile = jnp.repeat(smooth_coef.reshape(seams, PER_TILE), SLOT, axis=1)
    by_tile = jnp.pad(by_tile, ((0, 0), (0, LANES - SLOT * PER_TILE)))
    lane_coefs = jnp.where(inside, jnp.stack([by_tile, 1.0 - 4.0 * by_tile]), 0.0)
    lane_coefs = jnp.broadcast_to(lane_coefs[:, :, None, :], (2, seams, SUB, LANES))
    return call(
        seam_kernel,
        (1,),
        [
            smem(),
            whole(2, seams, SUB, LANES),
            whole(sents, extended, LANES),
            whole(sents, extended, LANES),
            whole(seams, rows, LANES),
            whole(seams, SUB, LANES),
            whole(parents, rows, columns),
        ],
        pl.BlockSpec(memory_space=pltpu.HBM),
        pltpu.HBM((parents, rows, columns), BF16),
        [
            pltpu.VMEM((seams, extended, LANES), F32),
            pltpu.VMEM((2, seams, extended // SUB, SUB, LANES), F32),
            pltpu.VMEM((parents, rows, columns), BF16),
            pltpu.SemaphoreType.DMA((seams,)),
        ],
    )(info, lane_coefs, column_even, column_odd, edge_core, edge_halo, main)


def shards(child_field, parent_old, level_map, intersection, thickness, smooth_coef, nest_mask):
    children, parents = child_field.shape[0], parent_old.shape[0]
    most = children - parents + 1
    ends = level_map[children - 1 : children + 1]
    crossing = jnp.max(ends * jnp.array([1, -1]) + jnp.array([2 - parents, parents]))

    def run(count):
        return lambda: feed_back(
            count, child_field, parent_old, intersection, thickness, level_map, smooth_coef, nest_mask
        )

    return lax.cond(crossing <= SMALL_RUNG, run(SMALL_RUNG), run(most))


def solution(mesh):
    in_specs = (P("lev", "gx", "gy"), P("lev", "gx", "gy"), P(), P(), P(), P("lev"), P("gx", "gy"))
    out_specs = P("lev", "gx", "gy")
    return jax.shard_map(shards, mesh=mesh, in_specs=in_specs, out_specs=out_specs, check_vma=False)
```

```python
import functools

import jax
import jax.numpy as jnp
from jax import lax
from jax.experimental import pallas as pl
from jax.experimental.pallas import tpu as pltpu
from jax.sharding import PartitionSpec as P

SMOOTH = 4
LANES = 128
SUB = 8
SLOT = 24
PER_TILE = 5
PER_SENT = 3
PER_SWEEP = 9
SMALL_RUNG = 1
ROW_BLOCK = 32
F32 = jnp.float32
BF16 = jnp.bfloat16
VMEM_MIB = 1 << 20


def pair_swap(x, axis, parity):
    route = []
    for low in range(parity, lax.axis_size(axis) - 1, 2):
        route += [(low, low + 1), (low + 1, low)]
    return lax.ppermute(x, axis, route)


def call(kernel, grid, in_specs, out_specs, out_shape, scratch=(), flops=1, limit=24):
    return pl.pallas_call(
        kernel,
        grid=grid,
        in_specs=in_specs,
        out_specs=out_specs,
        out_shape=out_shape,
        scratch_shapes=list(scratch),
        compiler_params=pltpu.CompilerParams(vmem_limit_bytes=limit * VMEM_MIB),
        cost_estimate=pl.CostEstimate(flops=flops, bytes_accessed=1 << 20, transcendentals=0),
    )


def smem():
    return pl.BlockSpec(memory_space=pltpu.SMEM)


def whole(*shape):
    return pl.BlockSpec(shape, lambda *_: (0,) * len(shape))


def deal_column(row, size):
    r = lax.broadcasted_iota(jnp.int32, (size, size), 0)
    c = lax.broadcasted_iota(jnp.int32, (size, size), 1)
    return jnp.sum(jnp.where(r == c, row, 0.0), axis=1, keepdims=True)


def share_columns(rows, size, total):
    rows = [row[...].astype(F32).reshape(1, size) for row in rows]
    begins, inside, thick = (deal_column(row, size) for row in rows)
    parent = lax.broadcasted_iota(jnp.int32, (size, LANES), 1).astype(F32)
    raw = jnp.where(parent == begins, inside * thick, 0.0)
    upper = jnp.minimum(begins + 1.0, total - 1.0)
    raw = raw + jnp.where(parent == upper, (1.0 - inside) * thick, 0.0)
    sums = jnp.where(parent < total, jnp.sum(raw, axis=0, keepdims=True), 1.0)
    normed = (raw / sums).astype(BF16).astype(F32)
    low = jnp.sum(jnp.where(parent == begins, normed, 0.0), axis=1, keepdims=True)
    high = jnp.sum(jnp.where(parent == begins + 1.0, normed, 0.0), axis=1, keepdims=True)
    return low, high


def remap_kernel(
    count, total, info, begins, levels, inside, thick, child, own, part, acc, low, high, held, sems
):
    children, parents = child.shape[0], own.shape[0]
    size, width = low.shape

    block = acc.shape[1]
    chunks = held.shape[1] // block

    def copy(i):
        rows = pl.ds(pl.multiple_of(i * block, block), block)
        return pltpu.make_async_copy(child.at[:, rows, :], held.at[:, rows, :], sems.at[i])

    for i in range(chunks):
        copy(i).start()
    below, above = share_columns((levels, inside, thick), size, total)
    low[...] = jnp.broadcast_to(below, low.shape)
    high[...] = jnp.broadcast_to(above, high.shape)
    slab = info[7]
    origin = slab * children
    trash = parents + count
    first = begins[origin] - slab * parents
    last = begins[origin + children - 1] - slab * parents

    def clear(p, carry):
        acc[p] = jnp.zeros(acc.shape[1:], F32)
        return carry

    lax.fori_loop(0, jnp.maximum(first, 0), clear, 0)
    untouched = jnp.where(slab == 0, last + 2, parents)
    end = parents + jnp.where(slab == 0, count, jnp.clip(first + count, 0, count))
    lax.fori_loop(untouched, end, clear, 0)

    def chunk(i, carry):
        copy(i).wait()
        rows = pl.ds(pl.multiple_of(i * block, block), block)

        def step(k, state):
            here, above = state
            level = begins[origin + k]
            rose = level != begins[jnp.maximum(origin + k - 1, 0)]
            value = held[k, rows, :].astype(F32)
            here = jnp.where(rose, above, here) + low[pl.ds(origin + k, 1), :] * value
            above = jnp.where(rose, 0.0, above) + high[pl.ds(origin + k, 1), :] * value
            place = level - slab * parents
            place = jnp.where(place >= 0, place, parents + count + place)
            acc[jnp.clip(place, 0, trash)] = here
            return here, above

        zero = jnp.zeros(acc.shape[1:], F32)
        here, above = lax.fori_loop(0, children, step, (zero, zero), unroll=4)
        acc[jnp.where(slab == 0, jnp.clip(last + 1, 0, trash), trash)] = above

        def keep(p, carry):
            own[p, rows, :] = acc[p].astype(BF16)
            return carry

        lax.fori_loop(0, parents, keep, 0, unroll=5)

        def pass_on(j, carry):
            part[j, rows, :] = acc[parents + j].astype(BF16)
            return carry

        lax.fori_loop(0, count, pass_on, 0)
        return carry

    lax.fori_loop(0, chunks, chunk, 0)


def blend_kernel(group, own, par, mask, field, old, sems):
    steps = own.shape[0] // group

    def copy(i):
        levels = pl.ds(i * group, group)
        return pltpu.make_async_copy(par.at[levels], old.at[levels], sems.at[i])

    for i in range(steps):
        copy(i).start()
    fed = mask[...] != 0

    def step(i, carry):
        copy(i).wait()
        for j in range(group):
            p = i * group + j
            field[p] = jnp.where(fed, own[p].astype(F32), old[p].astype(F32)).astype(BF16)
        return carry

    lax.fori_loop(0, steps, step, 0)


def rows_kernel(count, info, field_t, field_b, mask_t, mask_b, part_t, part_b, even, odd, top, bot):
    parents = field_t.shape[0]
    row = lax.broadcasted_iota(jnp.int32, field_t.shape[1:], 0)
    flip = info[0] == 1
    fed_t, fed_b = mask_t[...] != 0, mask_b[...] != 0

    def copy(p, carry):
        top[p] = field_t[p].astype(F32)
        bot[p] = field_b[p].astype(F32)
        return carry

    lax.fori_loop(0, parents, copy, 0, unroll=9)

    def add_partner(j, carry):
        p = info[2] + j
        top[p] += jnp.where(fed_t, part_t[j].astype(F32), 0.0)
        bot[p] += jnp.where(fed_b, part_b[j].astype(F32), 0.0)
        return carry

    lax.fori_loop(0, count, add_partner, 0)
    for m in range(even.shape[0]):
        p, q = 2 * m, min(2 * m + 1, parents - 1)
        first = jnp.where(row < SMOOTH, top[p], pltpu.roll(top[q], SMOOTH, 0))
        last = jnp.where(row < SMOOTH, pltpu.roll(bot[p], SMOOTH, 0), bot[q])
        even[m] = jnp.where(flip, first, last).astype(BF16)
        odd[m] = jnp.where(flip, last, first).astype(BF16)


def edge_kernel(count, info, field, mask, part, fixed, edge, sent):
    parents = field.shape[0]
    fed = mask[...] != 0

    def fix(j, carry):
        value = field[info[2] + j].astype(F32) + jnp.where(fed, part[j].astype(F32), 0.0)
        fixed[j] = value.astype(BF16)
        return carry

    lax.fori_loop(0, count, fix, 0)

    def load(p):
        value = field[p].astype(F32)
        for start, near in ((0, p < count), (parents - count, p >= parents - count)):
            if near:
                mine = info[2] == start
                value = jnp.where(mine, fixed[p - start].astype(F32), value)
        return value

    edges = make_edges(parents, load)
    for t, tile in enumerate(edges):
        edge[t] = tile.astype(BF16)
    for t, tile in enumerate(make_sent(edges)):
        sent[t] = tile.astype(BF16)


def make_edges(parents, load):
    tiles = []
    for t in range(pl.cdiv(parents, PER_TILE)):
        tile = None
        for j in range(min(PER_TILE, parents - t * PER_TILE)):
            value = load(t * PER_TILE + j)
            lane = lax.broadcasted_iota(jnp.int32, (value.shape[0], LANES), 1)
            both = jnp.where(lane < LANES // 2, value[:, :LANES], value[:, -LANES:])
            both = pltpu.roll(both, (SLOT * j + 8) % LANES, 1)
            tile = both if tile is None else jnp.where(lane >= SLOT * j, both, tile)
        tiles.append(jnp.where(lane % SLOT < 8, tile, pltpu.roll(tile, 8, 1)))
    return tiles


def make_sent(edges):
    tiles = []
    for q in range(pl.cdiv(len(edges), PER_SENT)):
        tile = None
        for u, edge in enumerate(edges[q * PER_SENT : (q + 1) * PER_SENT]):
            lane = lax.broadcasted_iota(jnp.int32, edge.shape, 1) % SLOT - 8 * u
            last = pltpu.roll(edge, (8 * u - 4) % LANES, 1)
            first = pltpu.roll(edge, (8 * u - 12) % LANES, 1)
            both = jnp.where(lane < 4, last, first)
            tile = both if tile is None else jnp.where(lane >= 0, both, tile)
        tiles.append(tile)
    return tiles


def halo_kernel(parents, info, even, odd, sent_core, halo, edge, sent):
    flip = info[0] == 1
    row = lax.broadcasted_iota(jnp.int32, halo.shape[1:], 0)

    def load(p):
        a, b = even[p // 2].astype(F32), odd[p // 2].astype(F32)
        after, before = jnp.where(flip, b, a), jnp.where(flip, a, b)
        if p % 2 == 0:
            before = pltpu.roll(before, SMOOTH, 0)
        else:
            after = pltpu.roll(after, SMOOTH, 0)
        value = jnp.where(row < SMOOTH, after, before)
        halo[p] = value.astype(BF16)
        return value

    edges = make_edges(parents, load)
    for t, tile in enumerate(edges):
        edge[t] = tile.astype(BF16)
    rows = sent_core.shape[1]
    sent[:, :rows, :] = sent_core[...]
    for t, tile in enumerate(make_sent(edges)):
        sent[t, rows:, :] = tile.astype(BF16)


def row_sweep(values, side_sum, scales, keeps):
    count = len(values)
    before = pltpu.roll(values[-1], 1, 0)
    after = pltpu.roll(values[0], SUB - 1, 0)
    out = []
    for i, value in enumerate(values):
        up = values[i - 1] if i > 0 else before
        down = values[i + 1] if i < count - 1 else after
        out.append(keeps[i] * value + scales[i] * ((up + down) + side_sum(i, value)))
    return out


def row_flags(info, count, rows):
    sub = lax.broadcasted_iota(jnp.int32, (SUB, LANES), 0)
    flags = []
    for i in range(count):
        r = (SUB - 1) * count + i - rows
        if r < 0:
            flags.append(None)
            continue
        inside = info[4] if r < SMOOTH else info[3]
        flags.append(jnp.where(sub == SUB - 1, inside.astype(F32), 1.0))
    return flags


def smooth_kernel(count, info, coefs, field, fixed, halo, out, left, right, work, near):
    levels, rows = left.shape[0], field.shape[1]
    deals = left.shape[1] // SUB
    flags = row_flags(info, deals, rows)
    flags = [None if f is None else jnp.concatenate([f, f], axis=1) for f in flags]
    r = lax.broadcasted_iota(jnp.int32, near.shape, 0)
    c = lax.broadcasted_iota(jnp.int32, near.shape, 1)
    near[...] = jnp.where(jnp.abs(r - c) == 1, 1.0, 0.0).astype(BF16)

    def group(g, carry):
        base = g * levels
        weights = []
        for p in range(levels):
            scale = coefs[base + p]
            keep = 1.0 - 4.0 * scale
            weights.append(
                (
                    [scale if f is None else scale * f for f in flags],
                    [keep if f is None else keep * f for f in flags],
                )
            )
            j = base + p - info[2]
            use_fixed = (j >= 0) & (j < count)
            j = jnp.clip(j, 0, count - 1)
            for ref, cut in ((left, slice(0, LANES)), (right, slice(LANES, 2 * LANES))):
                ref[p, :rows, :] = field[base + p, :, cut].astype(F32)

                @pl.when(use_fixed)
                def _():
                    ref[p, :rows, :] = fixed[j, :, cut].astype(F32)

                ref[p, rows:, :] = halo[base + p, :, cut].astype(F32)
            for i in range(deals):
                part = slice(SUB * i, SUB * i + SUB)
                work[0, p, part, :LANES] = left[p, pl.ds(i, SUB, stride=deals), :]
                work[0, p, part, LANES:] = right[p, pl.ds(i, SUB, stride=deals), :]
        for s in range(SMOOTH):
            for p in range(levels):
                first = p - p % PER_SENT
                if p == first:
                    flat = work[s % 2, p : p + PER_SENT].reshape(-1, 2 * LANES).astype(BF16)
                    side = jnp.dot(flat, near[...], preferred_element_type=F32)
                    side = side.reshape(PER_SENT, deals * SUB, 2 * LANES)
                values = [work[s % 2, p, SUB * i : SUB * i + SUB, :] for i in range(deals)]
                values = row_sweep(
                    values, lambda i, _: side[p - first, SUB * i : SUB * i + SUB, :], *weights[p]
                )
                for i, value in enumerate(values):
                    if s == SMOOTH - 1:
                        left[p, pl.ds(i, SUB, stride=deals), :] = value[:, :LANES]
                        right[p, pl.ds(i, SUB, stride=deals), :] = value[:, LANES:]
                    else:
                        work[(s + 1) % 2, p, SUB * i : SUB * i + SUB, :] = value
        for p in range(levels):
            out[base + p, :, :LANES] = left[p, :rows, :].astype(BF16)
            out[base + p, :, LANES:] = right[p, :rows, :].astype(BF16)
        return carry

    lax.fori_loop(0, field.shape[0] // levels, group, 0)


def seam_kernel(info, coefs, even, odd, core, edge, main, out, tiles, work, done, sems):
    total = tiles.shape[0]
    rows = core.shape[1]
    count = tiles.shape[1] // SUB
    flip = info[1] == 1
    flags = row_flags(info, count, rows)
    slot = lax.broadcasted_iota(jnp.int32, tiles.shape[1:], 1) % SLOT
    for q in range(even.shape[0]):
        a, b = even[q].astype(F32), odd[q].astype(F32)
        after, before = jnp.where(flip, b, a), jnp.where(flip, a, b)
        for u in range(min(PER_SENT, total - q * PER_SENT)):
            t = q * PER_SENT + u
            own = jnp.concatenate([core[t].astype(F32), edge[t].astype(F32)], axis=0)
            right = pltpu.roll(after, (4 - 8 * u) % LANES, 1)
            left = pltpu.roll(before, (12 - 8 * u) % LANES, 1)
            tile = jnp.where(slot < 12, right, left)
            tiles[t] = jnp.where((slot >= 8) & (slot < 16), tile, own)
    for t in range(total):
        for i in range(count):
            work[0, t, i] = tiles[t, pl.ds(i, SUB, stride=count), :]
    for s in range(SMOOTH):
        for t in range(total):
            scale = coefs[0, t]
            keep = coefs[1, t]
            scales = [scale if f is None else scale * f for f in flags]
            keeps = [keep if f is None else keep * f for f in flags]
            values = [work[s % 2, t, i] for i in range(count)]
            new = row_sweep(
                values,
                lambda _, x: pltpu.roll(x, 1, 1) + pltpu.roll(x, LANES - 1, 1),
                scales,
                keeps,
            )
            for i in range(count):
                if s < SMOOTH - 1:
                    work[(s + 1) % 2, t, i] = new[i]
                else:
                    tiles[t, pl.ds(i, SUB, stride=count), :] = new[i]

    group = main.shape[0] // total

    def copy(i):
        levels = pl.ds(i * group, group)
        return pltpu.make_async_copy(done.at[levels], out.at[levels], sems.at[i])

    def step(i, carry):
        seam = tiles[i, :rows, :]
        lane = lax.broadcasted_iota(jnp.int32, seam.shape, 1)
        seam = jnp.where(lane % SLOT < 8, seam, pltpu.roll(seam, LANES - 8, 1))
        for j in range(group):
            both = pltpu.roll(seam, (120 - SLOT * j) % LANES, 1)
            p = i * group + j
            a, b = main[p, :, :LANES].astype(F32), main[p, :, LANES:].astype(F32)
            done[p, :, :LANES] = jnp.where(lane < SMOOTH, both, a).astype(BF16)
            done[p, :, LANES:] = jnp.where(lane >= LANES - SMOOTH, both, b).astype(BF16)
        copy(i).start()
        return carry

    lax.fori_loop(0, total, step, 0)
    for i in range(total):
        copy(i).wait()


def device_facts(start):
    slab, gx, gy = lax.axis_index("lev"), lax.axis_index("gx"), lax.axis_index("gy")
    facts = [
        gx % 2,
        gy % 2,
        start,
        gx > 0,
        gx < lax.axis_size("gx") - 1,
        gy > 0,
        gy < lax.axis_size("gy") - 1,
        slab,
    ]
    return jnp.stack([jnp.asarray(fact, jnp.int32) for fact in facts])


def feed_back(count, child, parent, inside, thick, level_map, smooth_coef, mask):
    children, rows, columns = child.shape
    parents = parent.shape[0]
    total = parents * lax.axis_size("lev")
    size = level_map.shape[0]
    slab = lax.axis_index("lev")
    info = device_facts(jnp.where(slab == 0, parents - count, 0))
    block = ROW_BLOCK
    own, part = call(
        functools.partial(remap_kernel, count, total),
        (1,),
        [
            smem(), smem(), whole(size), whole(size), whole(size),
            pl.BlockSpec(memory_space=pltpu.HBM),
        ],
        [whole(parents, rows, columns), whole(count, rows, columns)],
        [
            jax.ShapeDtypeStruct((parents, rows, columns), BF16),
            jax.ShapeDtypeStruct((count, rows, columns), BF16),
        ],
        [
            pltpu.VMEM((parents + count + 1, block, columns), F32),
            pltpu.VMEM((size, columns), F32),
            pltpu.VMEM((size, columns), F32),
            pltpu.VMEM((children, rows, columns), BF16),
            pltpu.SemaphoreType.DMA((rows // block,)),
        ],
    )(info, level_map, level_map, inside, thick, child)
    part = pair_swap(part, "lev", 0)
    group = PER_TILE
    field = call(
        functools.partial(blend_kernel, group),
        (1,),
        [whole(parents, rows, columns), pl.BlockSpec(memory_space=pltpu.HBM), whole(rows, columns)],
        whole(parents, rows, columns),
        jax.ShapeDtypeStruct((parents, rows, columns), BF16),
        [
            pltpu.VMEM((parents, rows, columns), BF16),
            pltpu.SemaphoreType.DMA((parents // group,)),
        ],
        flops=1 << 34,
    )(own, parent, mask)

    ends = rows // SUB - 1

    def two(lead):
        return [
            pl.BlockSpec((lead, SUB, columns), lambda i: (0, 0, 0)),
            pl.BlockSpec((lead, SUB, columns), lambda i: (0, ends, 0)),
        ]

    packed = pl.cdiv(parents, 2)
    strip = jax.ShapeDtypeStruct((packed, SUB, columns), BF16)
    row_even, row_odd = call(
        functools.partial(rows_kernel, count),
        (1,),
        [
            smem(),
            *two(parents),
            pl.BlockSpec((SUB, columns), lambda i: (0, 0)),
            pl.BlockSpec((SUB, columns), lambda i: (ends, 0)),
            *two(count),
        ],
        [whole(packed, SUB, columns)] * 2,
        [strip, strip],
        [pltpu.VMEM((parents, SUB, columns), F32)] * 2,
    )(info, field, field, mask, mask, part, part)
    row_even = pair_swap(row_even, "gx", 0)
    row_odd = pair_swap(row_odd, "gx", 1)

    seams = pl.cdiv(parents, PER_TILE)
    sents = pl.cdiv(seams, PER_SENT)
    fixed, edge_core, sent_core = call(
        functools.partial(edge_kernel, count),
        (rows // block,),
        [
            smem(),
            pl.BlockSpec((parents, block, columns), lambda i: (0, i, 0)),
            pl.BlockSpec((block, columns), lambda i: (i, 0)),
            pl.BlockSpec((count, block, columns), lambda i: (0, i, 0)),
        ],
        [
            pl.BlockSpec((count, block, columns), lambda i: (0, i, 0)),
            pl.BlockSpec((seams, block, LANES), lambda i: (0, i, 0)),
            pl.BlockSpec((sents, block, LANES), lambda i: (0, i, 0)),
        ],
        [
            jax.ShapeDtypeStruct((count, rows, columns), BF16),
            jax.ShapeDtypeStruct((seams, rows, LANES), BF16),
            jax.ShapeDtypeStruct((sents, rows, LANES), BF16),
        ],
        flops=1 << 34,
    )(info, field, mask, part)

    extended = rows + SUB
    halo, edge_halo, sent = call(
        functools.partial(halo_kernel, parents),
        (1,),
        [smem(), whole(packed, SUB, columns), whole(packed, SUB, columns), whole(sents, rows, LANES)],
        [whole(parents, SUB, columns), whole(seams, SUB, LANES), whole(sents, extended, LANES)],
        [
            jax.ShapeDtypeStruct((parents, SUB, columns), BF16),
            jax.ShapeDtypeStruct((seams, SUB, LANES), BF16),
            jax.ShapeDtypeStruct((sents, extended, LANES), BF16),
        ],
    )(info, row_even, row_odd, sent_core)
    column_even = pair_swap(sent, "gy", 0)
    column_odd = pair_swap(sent, "gy", 1)

    group = PER_TILE
    main = call(
        functools.partial(smooth_kernel, count),
        (1,),
        [
            smem(), smem(),
            whole(parents, rows, columns),
            whole(count, rows, columns),
            whole(parents, SUB, columns),
        ],
        whole(parents, rows, columns),
        jax.ShapeDtypeStruct((parents, rows, columns), BF16),
        [pltpu.VMEM((PER_SWEEP, extended, LANES), F32)] * 2
        + [
            pltpu.VMEM((2, PER_SWEEP, extended, columns), F32),
            pltpu.VMEM((columns, columns), BF16),
        ],
        flops=1 << 34,
    )(info, smooth_coef, field, fixed, halo)

    return finish(info, smooth_coef, column_even, column_odd, edge_core, edge_halo, main)


def finish(info, smooth_coef, column_even, column_odd, edge_core, edge_halo, main):
    parents, rows, columns = main.shape
    seams, extended = edge_core.shape[0], column_even.shape[1]
    sents, group = column_even.shape[0], PER_TILE
    gy = lax.axis_index("gy")
    lane = jnp.arange(LANES, dtype=jnp.int32)
    place_in_slot = lane % SLOT
    inside = lane < SLOT * PER_TILE
    after = (place_in_slot >= 8) & (place_in_slot < 12)
    before = (place_in_slot >= 12) & (place_in_slot < 16)
    inside &= ~after | (gy < lax.axis_size("gy") - 1)
    inside &= ~before | (gy > 0)
    by_tile = jnp.repeat(smooth_coef.reshape(seams, PER_TILE), SLOT, axis=1)
    by_tile = jnp.pad(by_tile, ((0, 0), (0, LANES - SLOT * PER_TILE)))
    lane_coefs = jnp.where(inside, jnp.stack([by_tile, 1.0 - 4.0 * by_tile]), 0.0)
    lane_coefs = jnp.broadcast_to(lane_coefs[:, :, None, :], (2, seams, SUB, LANES))
    return call(
        seam_kernel,
        (1,),
        [
            smem(),
            whole(2, seams, SUB, LANES),
            whole(sents, extended, LANES),
            whole(sents, extended, LANES),
            whole(seams, rows, LANES),
            whole(seams, SUB, LANES),
            whole(parents, rows, columns),
        ],
        pl.BlockSpec(memory_space=pltpu.HBM),
        pltpu.HBM((parents, rows, columns), BF16),
        [
            pltpu.VMEM((seams, extended, LANES), F32),
            pltpu.VMEM((2, seams, extended // SUB, SUB, LANES), F32),
            pltpu.VMEM((parents, rows, columns), BF16),
            pltpu.SemaphoreType.DMA((seams,)),
        ],
    )(info, lane_coefs, column_even, column_odd, edge_core, edge_halo, main)


def shards(child_field, parent_old, level_map, intersection, thickness, smooth_coef, nest_mask):
    children, parents = child_field.shape[0], parent_old.shape[0]
    most = children - parents + 1
    ends = level_map[children - 1 : children + 1]
    crossing = jnp.max(ends * jnp.array([1, -1]) + jnp.array([2 - parents, parents]))

    def run(count):
        return lambda: feed_back(
            count, child_field, parent_old, intersection, thickness, level_map, smooth_coef, nest_mask
        )

    return lax.cond(crossing <= SMALL_RUNG, run(SMALL_RUNG), run(most))


def solution(mesh):
    in_specs = (P("lev", "gx", "gy"), P("lev", "gx", "gy"), P(), P(), P(), P("lev"), P("gx", "gy"))
    out_specs = P("lev", "gx", "gy")
    return jax.shard_map(shards, mesh=mesh, in_specs=in_specs, out_specs=out_specs, check_vma=False)
```
